32 devices in a mesh: replica: 8 (over y, x, core), shard: 4 (over z).
Axes of the slice: x: 2, y: 2, z: 4, core: 2. Of those that a mesh axis runs over, the one named last changes fastest.
Arguments:
- params: float32 [8, 64, 28672], P('replica', 'shard'), may hold values from -6 to 6
- first_moment: float32 [8, 64, 28672], P('replica', 'shard'), may hold values from -3 to 3
- second_moment: float32 [8, 64, 28672], P('replica', 'shard'), may hold values from 0.25 to 4
- grads: bfloat16 [4, 8, 64, 28672], P(None, 'replica', 'shard'), may hold values from -6 to 6
- push_weight: float32 [8], P('replica'), may hold values from 0.5 to 2
Outputs:
- final_weights: bfloat16 [8, 64, 28672], P('replica')
The draws below stay inside these ranges and needn't reach their ends.
All inputs are finite; a program needn't handle non-finite values.
Results may differ from the reference program's by a relative error of at most 0.001.
Values may be sent and summed in bfloat16 or wider, within the bound.
A program may use at most 64 MiB of HBM per device.

```python
import math
import jax
import jax.numpy as jnp

COLS = 28672
STEPS = 4
ROWS = 64
REPLICAS = 8


def steps_of(key, shape, pieces, low, top_value):
    level, own = 1.0, jax.random.fold_in(key, 6)
    for dim, blocks in pieces:
        draws = jnp.exp(jax.random.uniform(jax.random.fold_in(own, dim), (blocks,), jnp.float32, low / len(pieces), top_value / len(pieces)))
        level = level * jnp.repeat(draws, shape[dim] // blocks).reshape([-1 if axis == dim else 1 for axis in range(len(shape))])
    return level


def scatter_about(key, dims, spread, most, cuts=(), held_as=jnp.bfloat16):
    level = steps_of(key, dims, cuts, -0.22, 0.18) if cuts else 1.0
    array = jax.random.normal(key, dims, jnp.float32) * spread * level
    return jnp.minimum(jnp.maximum(array, -most), most).astype(held_as)


def setup_inputs(seed: int = 0) -> dict:
    key_list = jax.random.split(jax.random.key(seed), 6)
    return {
        "params": scatter_about(key_list[0], (REPLICAS, ROWS, COLS), 1.0, 6.0, ((0, 8), (1, 4)), jnp.float32),
        "first_moment": scatter_about(key_list[1], (REPLICAS, ROWS, COLS), 0.5, 3.0, ((0, 8), (1, 4)), jnp.float32),
        "second_moment": jnp.clip(jnp.exp(math.log(4.0) - 2.7725887 * jax.random.uniform(key_list[2], (REPLICAS, ROWS, COLS), jnp.float32) ** steps_of(key_list[2], (REPLICAS, ROWS, COLS), ((0, 8), (1, 4)), -0.2, 0.2)), 0.25, 4.0),
        "grads": scatter_about(key_list[3], (STEPS, REPLICAS, ROWS, COLS), 1.0, 6.0, ((1, 8), (2, 4))),
        "push_weight": jnp.clip(0.5 + 1.5 * jax.random.uniform(key_list[4], (REPLICAS,), jnp.float32) ** steps_of(key_list[4], (REPLICAS,), ((0, 8),), -0.2, 0.2), 0.5, 2.0),
    }


beta_one = 0.9
beta_two = 0.95
learn_rate = 0.1
decay_rate = 0.1
epsilon = 1e-08
adam_offset = 101

def reference(params, first_moment, second_moment, grads, push_weight):
    levels = REPLICAS.bit_length() - 1
    weight = push_weight
    numer = params * weight[:, None, None]
    for iteration in range(STEPS):
        distance = 2 ** (iteration % levels)
        count = adam_offset + iteration
        first_fix = 1.0 - beta_one ** count
        second_fix = 1.0 - beta_two ** count
        current = numer / weight[:, None, None]
        gradient = grads[iteration].astype(jnp.float32)
        first_moment = beta_one * first_moment + (1.0 - beta_one) * gradient
        second_moment = beta_two * second_moment + (1.0 - beta_two) * gradient * gradient
        update = first_moment / first_fix / (jnp.sqrt(second_moment / second_fix) + epsilon)
        current = current - learn_rate * (update + decay_rate * current)
        numer = current * weight[:, None, None]
        numer = 0.5 * numer + 0.5 * jnp.roll(numer, distance, axis=0)
        weight = 0.5 * weight + 0.5 * jnp.roll(weight, distance, axis=0)
    return (numer / weight[:, None, None]).astype(jnp.bfloat16)
```

```python
import functools

import jax
import jax.numpy as jnp
from jax import lax
from jax.experimental import pallas as pl
from jax.experimental.pallas import tpu as pltpu
from jax.sharding import PartitionSpec as P

STEPS = 4


beta_one = 0.9
beta_two = 0.95
learn_rate = 0.1
decay_rate = 0.1
epsilon = 1e-08
adam_offset = 101

CODE_SCALE = 8.0
LAG = 3
HOP_LAG = 2
CHUNKS = 28
PARTS = 1
EARLY = 2
LOAD_GROUP = 2
SUB = 2
MESH = pl.DeviceIdType.MESH


def plan_of(replicas):
    levels = replicas.bit_length() - 1
    distances = [2 ** (step % levels) for step in range(STEPS)]
    every = {2**level for level in range(levels)}
    plan = []
    for step, distance in enumerate(distances):
        later = set(distances[step + 1 :])
        if every <= later:
            continue
        above = {d for d in every if d > distance}
        plan.append((step, distance, above <= later))
    return plan


def mixes_of(replicas):
    levels = replicas.bit_length() - 1
    mixes = [{0: 1.0}]
    for step in range(STEPS):
        distance, mixed = 2 ** (step % levels), {}
        for k, share in mixes[-1].items():
            for back in (k, (k + distance) % replicas):
                mixed[back] = mixed.get(back, 0.0) + 0.5 * share
        mixes.append(mixed)
    return mixes


def encode(value):
    power = value * CODE_SCALE
    power = power * power
    power = power * power
    power = power * power
    power = power * power
    return jnp.where(value < 0.0, -power, power).astype(jnp.bfloat16)


def decode(code):
    code = code.astype(jnp.float32)
    size = jnp.exp(jnp.log(jnp.abs(code)) * (1.0 / 16.0)) * (1.0 / CODE_SCALE)
    return jnp.where(code < 0.0, -size, size)


def kernel(
    plan, mixes, replicas, shards, chunks, chunk, parts, sub, load_group,
    params_ref, first_ref, second_ref, grads_ref, weight_ref, out_ref,
    params, first, second, grads, weights, scales, acc, terms, early, sent, arrived, final,
    load_sem, wsend, wrecv, xsend, xrecv, zsend, zrecv, own_sem,
):
    me, z = lax.axis_index("replica"), lax.axis_index("shard")
    rows = params.shape[0]
    rounds = len(plan)
    ends = [step for step, _, _ in plan]
    keep = 1.0 - learn_rate * decay_rate
    width = chunk // parts
    small = [(p * width, width, p) for p in range(parts)]

    def whole(i):
        return pl.multiple_of(i * chunk, chunk), chunk, i + parts - 1

    def columns(piece):
        return pl.ds(piece[0], piece[1])

    def slab(index):
        return pl.ds(pl.multiple_of(index * rows, rows), rows)

    def peer(offset):
        return lax.rem(me + offset + replicas, replicas)

    barrier = pltpu.get_barrier_semaphore()
    for k in range(1, replicas):
        pl.semaphore_signal(barrier, inc=1, device_id={"replica": peer(k)}, device_id_type=MESH)

    @pl.when(z > 0)
    def _():
        pl.semaphore_signal(barrier, inc=1, device_id={"shard": z - 1}, device_id_type=MESH)

    @pl.when(z < shards - 1)
    def _():
        pl.semaphore_signal(barrier, inc=1, device_id={"shard": z + 1}, device_id_type=MESH)

    def loads(g):
        cols = pl.ds(pl.multiple_of(g * (load_group * chunk), chunk), load_group * chunk)
        return (
            pltpu.make_async_copy(params_ref.at[0, :, cols], params.at[:, cols], load_sem.at[0, g]),
            pltpu.make_async_copy(first_ref.at[0, :, cols], first.at[:, cols], load_sem.at[1, g]),
            pltpu.make_async_copy(second_ref.at[0, :, cols], second.at[:, cols], load_sem.at[2, g]),
            pltpu.make_async_copy(grads_ref.at[:, 0, :, cols], grads.at[:, :, cols], load_sem.at[3, g]),
        )

    @pl.loop(0, chunks // load_group)
    def _(g):
        for copy in loads(g):
            copy.start()

    weights[me] = jnp.full(weights.shape[1:], weight_ref[0], jnp.float32)
    ends_of_line = jnp.where(z > 0, 1, 0) + jnp.where(z < shards - 1, 1, 0)
    pl.semaphore_wait(barrier, replicas - 1 + ends_of_line)

    def weight_copy(k, owner):
        return pltpu.make_async_remote_copy(
            src_ref=weights.at[owner], dst_ref=weights.at[owner],
            send_sem=wsend.at[k - 1], recv_sem=wrecv.at[k - 1],
            device_id={"replica": peer(k)}, device_id_type=MESH,
        )

    for k in range(1, replicas):
        weight_copy(k, me).start()

    def wide(tile):
        tile = jnp.concatenate([tile] * (rows // tile.shape[0]), axis=0) if rows > tile.shape[0] else tile[:rows]
        return jnp.concatenate([tile] * (sub // tile.shape[1]), axis=1)

    heard = set()

    def mixed(level):
        total = None
        for k, share in sorted(mixes[level].items()):
            if k and k not in heard:
                weight_copy(k, peer(-k)).wait_recv()
                heard.add(k)
            part = share * weights[peer(-k)]
            total = part if total is None else total + part
        return total

    def scale_of(step):
        end = min(e for e in ends if e >= step)
        scales[1 + step] = wide(mixed(step) * (learn_rate * keep ** (end - step)))

    def exchange(k, piece):
        _, distance, swap = plan[k]
        if swap:
            to = me + distance - 2 * distance * lax.rem(me // distance, 2)
        else:
            to = peer(distance)
        cols = slice(None) if piece is None else columns(piece)
        return pltpu.make_async_remote_copy(
            src_ref=sent.at[k, :, cols], dst_ref=arrived.at[k, :, cols],
            send_sem=xsend.at[k], recv_sem=xrecv.at[k, 0 if piece is None else piece[2]],
            device_id={"replica": to}, device_id_type=MESH,
        )

    def gather(way, hop, piece):
        sign = 1 - 2 * way
        cols, index = slice(None) if piece is None else columns(piece), z - sign * hop
        target = out_ref.at[0, slab(index), cols]
        return pltpu.make_async_remote_copy(
            src_ref=final.at[:, cols] if hop == 0 else target, dst_ref=target,
            send_sem=zsend.at[way, hop], recv_sem=zrecv.at[way, hop, 0 if piece is None else piece[2]],
            device_id={"shard": z + sign}, device_id_type=MESH,
        )

    def gathered(way, hop, piece):
        sign = 1 - 2 * way
        target = out_ref.at[0, slab(z - sign * hop), columns(piece)]
        return pltpu.make_async_remote_copy(
            src_ref=target, dst_ref=target,
            send_sem=zsend.at[way, hop - 1], recv_sem=zrecv.at[way, hop - 1, piece[2]],
            device_id={"shard": z - sign}, device_id_type=MESH,
        )

    def has_source(way, hop):
        return z >= hop if way == 0 else z + hop < shards

    def has_target(way):
        return z < shards - 1 if way == 0 else z > 0

    def own(piece):
        cols = slice(None) if piece is None else columns(piece)
        return pltpu.make_async_copy(final.at[:, cols], out_ref.at[0, slab(z), cols], own_sem)

    def adam(cols, known):
        m, v = first[:, cols], second[:, cols]
        total = scales[0] * params[:, cols]
        for step in range(STEPS):
            g = grads[step, :, cols].astype(jnp.float32)
            count = adam_offset + step
            m = beta_one * m + (1.0 - beta_one) * g
            v = beta_two * v + (1.0 - beta_two) * g * g
            fixed = jnp.sqrt(v * (1.0 / (1.0 - beta_two**count))) + epsilon
            update = m * (1.0 / (1.0 - beta_one**count)) / fixed
            if step > ends[0]:
                terms[step - ends[0] - 1, :, cols] = update
            elif step < known:
                total = total - update * scales[1 + step]
            else:
                early[step - known, :, cols] = update
        return total

    def tiles(piece):
        for j in range(piece[1] // sub):
            yield pl.ds(pl.multiple_of(piece[0] + j * sub, sub), sub)

    def first_half(piece):
        for cols in tiles(piece):
            acc[:, cols] = adam(cols, 1)

    def second_half(piece):
        for cols in tiles(piece):
            total = acc[:, cols]
            for step in range(1, ends[0] + 1):
                total = total - early[step - 1, :, cols] * scales[1 + step]
            acc[:, cols] = total
            sent[0, :, cols] = encode(total)
        exchange(0, piece).start()

    def start_round(piece):
        for cols in tiles(piece):
            total = adam(cols, STEPS)
            acc[:, cols] = total
            sent[0, :, cols] = encode(total)
        exchange(0, piece).start()

    def next_round(k, piece):
        exchange(k - 1, piece).wait_recv()
        for cols in tiles(piece):
            both = acc[:, cols] + decode(arrived[k - 1, :, cols])
            if k < rounds:
                both = both * (0.5 * keep ** (ends[k] - ends[k - 1])) - terms[k - 1, :, cols] * scales[1 + ends[k]]
                acc[:, cols] = both
                sent[k, :, cols] = encode(both)
            else:
                final[:, cols] = (both * scales[1 + STEPS]).astype(jnp.bfloat16)
        if k < rounds:
            exchange(k, piece).start()
        else:
            for way in range(2):
                pl.when(has_target(way))(lambda way=way: gather(way, 0, piece).start())
            own(piece).start()

    def pass_on(hop, piece):
        for way in range(2):

            @pl.when(jnp.logical_and(has_target(way), has_source(way, hop)))
            def _(way=way):
                gathered(way, hop, piece).wait_recv()
                gather(way, hop, piece).start()

    def wait_loads(i):
        @pl.when(lax.rem(i, load_group) == 0)
        def _():
            for copy in loads(i // load_group):
                copy.wait()

    scales[0] = wide(mixed(0) * keep ** (ends[0] + 1))
    scale_of(0)
    for i in range(EARLY):
        if i % load_group == 0:
            for copy in loads(i // load_group):
                copy.wait()
        for piece in small if i == 0 else [whole(i)]:
            first_half(piece)
    for step in range(1, ends[0] + 1):
        scale_of(step)
    for i in range(EARLY):
        for piece in small if i == 0 else [whole(i)]:
            second_half(piece)
    wait_loads(EARLY)
    start_round(whole(EARLY))
    for step in range(ends[0] + 1, STEPS):
        scale_of(step)
    scales[1 + STEPS] = wide(0.5 / mixed(STEPS))

    hops = max(shards - 2, 0)
    last = rounds * LAG

    @pl.loop(EARLY + 1, chunks + last + hops * HOP_LAG)
    def _(t):
        def at(delay, act, low=0):
            i = t - delay
            if low == 0 and parts > 1:

                @pl.when(i == 0)
                def _():
                    for piece in small:
                        act(piece)

                low = 1

            @pl.when(jnp.logical_and(i >= low, i < chunks))
            def _():
                act(whole(i))

        @pl.when(t < chunks)
        def _():
            wait_loads(t)
            start_round(whole(t))

        for k in range(1, rounds + 1):
            at(k * LAG, functools.partial(next_round, k))
        for hop in range(1, hops + 1):
            at(last + hop * HOP_LAG, functools.partial(pass_on, hop))

    for way in range(2):

        @pl.when(jnp.logical_not(has_target(way)))
        def _(way=way):
            def drain(piece):
                for hop in range(1, shards):
                    pl.when(has_source(way, hop))(lambda hop=hop: gathered(way, hop, piece).wait_recv())

            for piece in small:
                drain(piece)

            @pl.loop(1, chunks)
            def _(i):
                drain(whole(i))

    for k in range(1, replicas):
        weight_copy(k, me).wait_send()
    for k in range(rounds):
        exchange(k, None).wait_send()
    own(None).wait()
    for way in range(2):
        for hop in range(shards - 1):

            @pl.when(jnp.logical_and(has_target(way), has_source(way, hop)))
            def _(way=way, hop=hop):
                gather(way, hop, None).wait_send()


def per_device(params, first_moment, second_moment, grads, push_weight):
    replicas, shards = lax.axis_size("replica"), lax.axis_size("shard")
    _, rows, cols = params.shape
    units = cols // 128
    chunks = max(n for n in range(1, CHUNKS + 1) if units % n == 0)
    chunk = cols // chunks
    parts = PARTS if chunk % (128 * PARTS) == 0 else 1
    sub = max(128 * n for n in range(1, SUB + 1) if (chunk // parts) % (128 * n) == 0)
    load_group = LOAD_GROUP if chunks % LOAD_GROUP == 0 else 1
    plan, mixes = plan_of(replicas), mixes_of(replicas)
    rounds = len(plan)
    pieces = chunks + parts - 1
    f32, bf16, dma = jnp.float32, jnp.bfloat16, pltpu.SemaphoreType.DMA
    anywhere = pl.BlockSpec(memory_space=pl.ANY)
    body = functools.partial(kernel, plan, mixes, replicas, shards, chunks, chunk, parts, sub, load_group)
    hops = max(shards - 1, 1)
    large = (params, first_moment, second_moment, grads)
    large = tuple(pltpu.with_memory_space_constraint(x, pltpu.HBM) for x in large)
    return pl.pallas_call(
        body,
        out_shape=jax.ShapeDtypeStruct((1, rows * shards, cols), bf16),
        in_specs=[anywhere] * 4 + [pl.BlockSpec(memory_space=pltpu.SMEM)],
        out_specs=anywhere,
        scratch_shapes=[
            pltpu.VMEM((rows, cols), f32),
            pltpu.VMEM((rows, cols), f32),
            pltpu.VMEM((rows, cols), f32),
            pltpu.VMEM((STEPS, rows, cols), bf16),
            pltpu.VMEM((replicas, 8, 128), f32),
            pltpu.VMEM((STEPS + 2, rows, sub), f32),
            pltpu.VMEM((rows, cols), f32),
            pltpu.VMEM((max(rounds - 1, 1), rows, cols), f32),
            pltpu.VMEM((max(plan[0][0], 1), rows, EARLY * chunk), f32),
            pltpu.VMEM((rounds, rows, cols), bf16),
            pltpu.VMEM((rounds, rows, cols), bf16),
            pltpu.VMEM((rows, cols), bf16),
            dma((4, chunks // load_group)),
            dma((replicas - 1,)),
            dma((replicas - 1,)),
            dma((rounds,)),
            dma((rounds, pieces)),
            dma((2, hops)),
            dma((2, hops, pieces)),
            dma,
        ],
        compiler_params=pltpu.CompilerParams(
            collective_id=0, has_side_effects=True, vmem_limit_bytes=48 * 1024 * 1024
        ),
    )(*large, push_weight)


def solution(mesh):
    return jax.shard_map(
        per_device,
        mesh=mesh,
        in_specs=(
            P("replica", "shard", None),
            P("replica", "shard", None),
            P("replica", "shard", None),
            P(None, "replica", "shard", None),
            P("replica"),
        ),
        out_specs=P("replica", None, None),
        check_vma=False,
    )
```

```python
import functools

import jax
import jax.numpy as jnp
from jax import lax
from jax.experimental import pallas as pl
from jax.experimental.pallas import tpu as pltpu
from jax.sharding import PartitionSpec as P

STEPS = 4


beta_one = 0.9
beta_two = 0.95
learn_rate = 0.1
decay_rate = 0.1
epsilon = 1e-08
adam_offset = 101

CODE_SCALE = 8.0
GAP_SCALE = 16.0
LAG = 3
HOP_LAG = 2
CHUNKS = 28
OPEN_LAG = 18
FOLD_LAG = 2
FULL_TAIL = 3
EARLY = 2
LOAD_GROUP = 2
SUB = 2
MESH = pl.DeviceIdType.MESH


def plan_of(replicas):
    levels = replicas.bit_length() - 1
    distances = [2 ** (step % levels) for step in range(STEPS)]
    every = {2**level for level in range(levels)}
    plan = []
    for step, distance in enumerate(distances):
        later = set(distances[step + 1 :])
        if every <= later:
            continue
        above = {d for d in every if d > distance}
        plan.append((step, distance, above <= later))
    return plan


def mixes_of(replicas):
    levels = replicas.bit_length() - 1
    mixes = [{0: 1.0}]
    for step in range(STEPS):
        distance, mixed = 2 ** (step % levels), {}
        for k, share in mixes[-1].items():
            for back in (k, (k + distance) % replicas):
                mixed[back] = mixed.get(back, 0.0) + 0.5 * share
        mixes.append(mixed)
    return mixes


def encode(value, scale=CODE_SCALE):
    power = value * scale
    power = power * power
    power = power * power
    power = power * power
    power = power * power
    return jnp.where(value < 0.0, -power, power).astype(jnp.bfloat16)


def decode(code, scale=CODE_SCALE):
    code = code.astype(jnp.float32)
    size = jnp.exp(jnp.log(jnp.abs(code)) * (1.0 / 16.0)) * (1.0 / scale)
    return jnp.where(code < 0.0, -size, size)


def kernel(
    plan, mixes, replicas, shards, chunks, chunk, sub, load_group, spares,
    params_ref, first_ref, second_ref, grads_ref, weight_ref, out_ref,
    params, first, second, grads, weights, scales, acc, terms, early, sent, arrived, final,
    load_sem, wsend, wrecv, xsend, xrecv, zsend, zrecv,
    codes=None, extra=None, hold=None, gap=None, gaps=None,
    rsend=None, rrecv=None, gsend=None, grecv=None,
):
    me, z = lax.axis_index("replica"), lax.axis_index("shard")
    rows = params.shape[0]
    rounds = len(plan)
    ends = [step for step, _, _ in plan]
    keep = 1.0 - learn_rate * decay_rate
    coded = spares > 0
    side, column, line = lax.rem(me, 2), lax.rem(me // 2, 2), me // 4
    foreign = shards - 1

    def columns(i):
        return pl.ds(pl.multiple_of(i * chunk, chunk), chunk)

    def spread(count):
        return pl.ds(0, count * chunk)

    def at_end(z):
        return jnp.logical_or(z == 0, z == shards - 1)

    def spared(i):
        return jnp.logical_and(i >= 1, i <= 4 * spares)

    def same_column(i):
        return lax.rem(i, 2) == column

    def same_line(i):
        return lax.rem(i // 2, 2) == line

    def everything(*tests):
        return functools.reduce(jnp.logical_and, tests)

    def lacking(i):
        return everything(spared(i), side == 1, same_column(i), same_line(i))

    def slab(index):
        return pl.ds(pl.multiple_of(index * rows, rows), rows)

    def peer(offset):
        return lax.rem(me + offset + replicas, replicas)

    barrier = pltpu.get_barrier_semaphore()
    for k in range(1, replicas):
        pl.semaphore_signal(barrier, inc=1, device_id={"replica": peer(k)}, device_id_type=MESH)

    @pl.when(z > 0)
    def _():
        pl.semaphore_signal(barrier, inc=1, device_id={"shard": z - 1}, device_id_type=MESH)

    @pl.when(z < shards - 1)
    def _():
        pl.semaphore_signal(barrier, inc=1, device_id={"shard": z + 1}, device_id_type=MESH)

    def loads(g):
        cols = pl.ds(pl.multiple_of(g * (load_group * chunk), chunk), load_group * chunk)
        return (
            pltpu.make_async_copy(params_ref.at[0, :, cols], params.at[:, cols], load_sem.at[0, g]),
            pltpu.make_async_copy(first_ref.at[0, :, cols], first.at[:, cols], load_sem.at[1, g]),
            pltpu.make_async_copy(second_ref.at[0, :, cols], second.at[:, cols], load_sem.at[2, g]),
            pltpu.make_async_copy(grads_ref.at[:, 0, :, cols], grads.at[:, :, cols], load_sem.at[3, g]),
        )

    @pl.loop(0, chunks // load_group)
    def _(g):
        for copy in loads(g):
            copy.start()

    weights[me] = jnp.full(weights.shape[1:], weight_ref[0], jnp.float32)
    ends_of_line = jnp.where(z > 0, 1, 0) + jnp.where(z < shards - 1, 1, 0)
    pl.semaphore_wait(barrier, replicas - 1 + ends_of_line)

    def weight_copy(k, owner):
        return pltpu.make_async_remote_copy(
            src_ref=weights.at[owner], dst_ref=weights.at[owner],
            send_sem=wsend.at[k - 1], recv_sem=wrecv.at[k - 1],
            device_id={"replica": peer(k)}, device_id_type=MESH,
        )

    for k in range(1, replicas):
        weight_copy(k, me).start()

    def wide(tile):
        tile = jnp.concatenate([tile] * (rows // tile.shape[0]), axis=0) if rows > tile.shape[0] else tile[:rows]
        return jnp.concatenate([tile] * (sub // tile.shape[1]), axis=1)

    heard = set()

    def mixed(level):
        total = None
        for k, share in sorted(mixes[level].items()):
            if k and k not in heard:
                weight_copy(k, peer(-k)).wait_recv()
                heard.add(k)
            part = share * weights[peer(-k)]
            total = part if total is None else total + part
        return total

    def scale_of(step):
        end = min(e for e in ends if e >= step)
        scales[1 + step] = wide(mixed(step) * (learn_rate * keep ** (end - step)))

    def exchange(k, i):
        _, distance, swap = plan[k]
        if swap:
            to = me + distance - 2 * distance * lax.rem(me // distance, 2)
        else:
            to = peer(distance)
        cols = slice(None) if i is None else columns(i)
        return pltpu.make_async_remote_copy(
            src_ref=sent.at[k, :, cols], dst_ref=arrived.at[k, :, cols],
            send_sem=xsend.at[k], recv_sem=xrecv.at[k, 0 if i is None else i],
            device_id={"replica": to}, device_id_type=MESH,
        )

    def ring(index, cols):
        return codes.at[slab(index), cols] if coded else out_ref.at[0, slab(index), cols]

    def gather(way, hop, i, count=None):
        sign = 1 - 2 * way
        cols, index = columns(i) if count is None else spread(count), z - sign * hop
        target = ring(index, cols)
        return pltpu.make_async_remote_copy(
            src_ref=final.at[:, cols] if hop == 0 else target, dst_ref=target,
            send_sem=zsend.at[way, hop], recv_sem=zrecv.at[way, hop, i],
            device_id={"shard": z + sign}, device_id_type=MESH,
        )

    def gathered(way, hop, i):
        sign = 1 - 2 * way
        target = ring(z - sign * hop, columns(i))
        return pltpu.make_async_remote_copy(
            src_ref=target, dst_ref=target,
            send_sem=zsend.at[way, hop - 1], recv_sem=zrecv.at[way, hop - 1, i],
            device_id={"shard": z - sign}, device_id_type=MESH,
        )

    def outward(way):
        return z == shards - 2 if way == 0 else z == 1

    def sends(way, hop, i):
        holds = jnp.logical_and(has_target(way), has_source(way, hop))
        if coded:
            holds = jnp.logical_and(holds, jnp.logical_not(jnp.logical_and(outward(way), lacking(i))))
        return holds

    def has_source(way, hop):
        return z >= hop if way == 0 else z + hop < shards

    def has_target(way):
        return z < shards - 1 if way == 0 else z > 0

    def adam(cols, known):
        m, v = first[:, cols], second[:, cols]
        total = scales[0] * params[:, cols]
        for step in range(STEPS):
            g = grads[step, :, cols].astype(jnp.float32)
            count = adam_offset + step
            m = beta_one * m + (1.0 - beta_one) * g
            v = beta_two * v + (1.0 - beta_two) * g * g
            fixed = jnp.sqrt(v * (1.0 / (1.0 - beta_two**count))) + epsilon
            update = m * (1.0 / (1.0 - beta_one**count)) / fixed
            if step > ends[0]:
                terms[step - ends[0] - 1, :, cols] = update
            elif step < known:
                total = total - update * scales[1 + step]
            else:
                early[step - known, :, cols] = update
        return total

    def tiles(i):
        for j in range(chunk // sub):
            yield pl.ds(pl.multiple_of(i * chunk + j * sub, sub), sub)

    def first_half(i):
        for cols in tiles(i):
            acc[:, cols] = adam(cols, 1)

    def second_half(i):
        for cols in tiles(i):
            total = acc[:, cols]
            for step in range(1, ends[0] + 1):
                total = total - early[step - 1, :, cols] * scales[1 + step]
            acc[:, cols] = total
            sent[0, :, cols] = encode(total)
        exchange(0, i).start()

    def start_round(i):
        for cols in tiles(i):
            total = adam(cols, STEPS)
            acc[:, cols] = total
            sent[0, :, cols] = encode(total)
        exchange(0, i).start()

    def next_round(k, i):
        exchange(k - 1, i).wait_recv()
        for cols in tiles(i):
            both = acc[:, cols] + decode(arrived[k - 1, :, cols])
            if k < rounds:
                both = both * (0.5 * keep ** (ends[k] - ends[k - 1])) - terms[k - 1, :, cols] * scales[1 + ends[k]]
                acc[:, cols] = both
                sent[k, :, cols] = encode(both)
            else:
                done = (both * scales[1 + STEPS]).astype(jnp.bfloat16)
                out_ref[0, slab(z), cols] = done
                final[:, cols] = encode(0.5 * both) if coded else done
        if k < rounds:
            exchange(k, i).start()
        else:
            for way in range(2):
                pl.when(sends(way, 0, i))(lambda way=way: gather(way, 0, i).start())

    def pass_on(hop, i):
        for way in range(2):

            @pl.when(jnp.logical_and(has_target(way), has_source(way, hop)))
            def _(way=way):
                gathered(way, hop, i).wait_recv()

            @pl.when(sends(way, hop, i))
            def _(way=way):
                gather(way, hop, i).start()

    def collect(i):
        for way in range(2):

            @pl.when(jnp.logical_not(has_target(way)))
            def _(way=way):
                for hop in range(1, shards):
                    gathered(way, hop, i).wait_recv()

    def abroad(j):
        return slab(j + jnp.where(j >= z, 1, 0))

    def relay(i, count=None):
        cols = columns(i) if count is None else spread(count)
        start = jnp.where(z == 0, rows, 0)
        return pltpu.make_async_remote_copy(
            src_ref=codes.at[pl.ds(pl.multiple_of(start, rows), foreign * rows), cols], dst_ref=extra.at[:, cols],
            send_sem=rsend, recv_sem=rrecv.at[i],
            device_id={"replica": me + 1 - 2 * side}, device_id_type=MESH,
        )

    def share(hop, i, count=None):
        cols = columns(i) if count is None else spread(count)
        to = me + 2 - 4 * column if hop else me + 4 - 8 * line
        return pltpu.make_async_remote_copy(
            src_ref=gap.at[:, cols], dst_ref=gaps.at[hop, :, cols],
            send_sem=gsend.at[hop], recv_sem=grecv.at[hop, i],
            device_id={"replica": to}, device_id_type=MESH,
        )

    def foreign_tiles(i):
        for j in range(foreign):
            for cols, held in zip(tiles(i), tiles(lax.rem(i, 4))):
                yield pl.ds(j * rows, rows), abroad(j), cols, held

    def put(where, cols, value):
        out_ref[0, where, cols] = (value * scales[2 + STEPS]).astype(jnp.bfloat16)

    def open_slabs(i):
        folds = jnp.logical_and(at_end(z), spared(i))

        @pl.when(jnp.logical_and(at_end(z), jnp.logical_not(lacking(i))))
        def _():
            collect(i)

        @pl.when(jnp.logical_and(folds, side == 0))
        def _():
            relay(i).start()

        @pl.when(jnp.logical_not(jnp.logical_and(folds, side == 1)))
        def _():
            for _, where, cols, _ in foreign_tiles(i):
                put(where, cols, decode(codes[where, cols]))

    def begin_fold(i):
        @pl.when(everything(at_end(z), spared(i), side == 1, jnp.logical_not(lacking(i))))
        def _():
            relay(i).wait_recv()
            for at, where, cols, held in foreign_tiles(i):
                value = decode(codes[where, cols])
                put(where, cols, value)
                apart = decode(extra[at, cols]) - value
                hold[at, held] = apart
                gap[at, cols] = encode(apart, GAP_SCALE)

            @pl.when(jnp.logical_not(same_line(i)))
            def _():
                share(0, i).start()

    def join_fold(i):
        @pl.when(everything(at_end(z), spared(i), side == 1, same_line(i), jnp.logical_not(same_column(i))))
        def _():
            share(0, i).wait_recv()
            for at, _, cols, held in foreign_tiles(i):
                gap[at, cols] = encode(hold[at, held] + decode(gaps[0, at, cols], GAP_SCALE), GAP_SCALE)
            share(1, i).start()

    def end_fold(i):
        @pl.when(jnp.logical_and(at_end(z), lacking(i)))
        def _():
            relay(i).wait_recv()
            share(0, i).wait_recv()
            share(1, i).wait_recv()
            for at, where, cols, _ in foreign_tiles(i):
                apart = decode(gaps[0, at, cols], GAP_SCALE) + decode(gaps[1, at, cols], GAP_SCALE)
                put(where, cols, decode(extra[at, cols]) + apart)

    def wait_loads(i):
        @pl.when(lax.rem(i, load_group) == 0)
        def _():
            for copy in loads(i // load_group):
                copy.wait()

    scales[0] = wide(mixed(0) * keep ** (ends[0] + 1))
    scale_of(0)
    for i in range(EARLY):
        if i % load_group == 0:
            for copy in loads(i // load_group):
                copy.wait()
        first_half(i)
    for step in range(1, ends[0] + 1):
        scale_of(step)
    for i in range(EARLY):
        second_half(i)
    wait_loads(EARLY)
    start_round(EARLY)
    for step in range(ends[0] + 1, STEPS):
        scale_of(step)
    scales[1 + STEPS] = wide(0.5 / mixed(STEPS))
    scales[2 + STEPS] = wide(1.0 / mixed(STEPS))

    hops = max(shards - 2, 0)
    last = rounds * LAG
    late = max(last + hops * HOP_LAG, OPEN_LAG)

    @pl.loop(EARLY + 1, chunks + (late + 1 + 2 * FOLD_LAG if coded else last + hops * HOP_LAG))
    def _(t):
        def at(delay, act):
            i = t - delay

            @pl.when(jnp.logical_and(i >= 0, i < chunks))
            def _():
                act(i)

        @pl.when(t < chunks)
        def _():
            wait_loads(t)
            start_round(t)

        for k in range(1, rounds + 1):
            at(k * LAG, functools.partial(next_round, k))
        for hop in range(1, hops + 1):
            at(last + hop * HOP_LAG, functools.partial(pass_on, hop))
        if coded:
            at(late, open_slabs)
            at(late + 1, begin_fold)
            at(late + 1 + FOLD_LAG, join_fold)
            at(late + 1 + 2 * FOLD_LAG, end_fold)

    if not coded:

        @pl.loop(0, chunks)
        def _(i):
            collect(i)

    for k in range(1, replicas):
        weight_copy(k, me).wait_send()
    for k in range(rounds):
        exchange(k, None).wait_send()
    for way in range(2):
        for hop in range(shards - 1):
            holds = jnp.logical_and(has_target(way), has_source(way, hop))
            if coded:
                less = jnp.logical_and(outward(way), side == 1)

                @pl.when(jnp.logical_and(holds, less))
                def _(way=way, hop=hop):
                    gather(way, hop, 0, chunks - spares).wait_send()

                holds = jnp.logical_and(holds, jnp.logical_not(less))

            @pl.when(holds)
            def _(way=way, hop=hop):
                gather(way, hop, 0, chunks).wait_send()

    if coded:

        @pl.when(jnp.logical_and(at_end(z), side == 0))
        def _():
            relay(0, 4 * spares).wait_send()

        @pl.when(jnp.logical_and(at_end(z), side == 1))
        def _():
            share(0, 0, 2 * spares).wait_send()
            share(1, 0, spares).wait_send()


def per_device(params, first_moment, second_moment, grads, push_weight):
    replicas, shards = lax.axis_size("replica"), lax.axis_size("shard")
    _, rows, cols = params.shape
    units = cols // 128
    chunks = max(n for n in range(1, CHUNKS + 1) if units % n == 0)
    chunk = cols // chunks
    sub = max(128 * n for n in range(1, SUB + 1) if chunk % (128 * n) == 0)
    load_group = LOAD_GROUP if chunks % LOAD_GROUP == 0 else 1
    plan, mixes = plan_of(replicas), mixes_of(replicas)
    rounds = len(plan)
    alternate = replicas == 8 and plan[-1][1] == 1 and not plan[-1][2] and shards > 2
    spares = max(chunks - 1 - FULL_TAIL, 0) // 4 if alternate else 0
    f32, bf16, dma = jnp.float32, jnp.bfloat16, pltpu.SemaphoreType.DMA
    anywhere = pl.BlockSpec(memory_space=pl.ANY)
    body = functools.partial(kernel, plan, mixes, replicas, shards, chunks, chunk, sub, load_group, spares)
    hops = max(shards - 1, 1)
    large = (params, first_moment, second_moment, grads)
    large = tuple(pltpu.with_memory_space_constraint(x, pltpu.HBM) for x in large)
    apart = (shards - 1) * rows
    folding = (
        pltpu.VMEM((shards * rows, cols), bf16),
        pltpu.VMEM((apart, cols), bf16),
        pltpu.VMEM((apart, 4 * chunk), f32),
        pltpu.VMEM((apart, cols), bf16),
        pltpu.VMEM((2, apart, cols), bf16),
        dma,
        dma((chunks,)),
        dma((2,)),
        dma((2, chunks)),
    )
    return pl.pallas_call(
        body,
        out_shape=jax.ShapeDtypeStruct((1, rows * shards, cols), bf16),
        in_specs=[anywhere] * 4 + [pl.BlockSpec(memory_space=pltpu.SMEM)],
        out_specs=pl.BlockSpec(memory_space=pltpu.VMEM),
        scratch_shapes=[
            pltpu.VMEM((rows, cols), f32),
            pltpu.VMEM((rows, cols), f32),
            pltpu.VMEM((rows, cols), f32),
            pltpu.VMEM((STEPS, rows, cols), bf16),
            pltpu.VMEM((replicas, 8, 128), f32),
            pltpu.VMEM((STEPS + 3, rows, sub), f32),
            pltpu.VMEM((rows, cols), f32),
            pltpu.VMEM((max(rounds - 1, 1), rows, cols), f32),
            pltpu.VMEM((max(plan[0][0], 1), rows, EARLY * chunk), f32),
            pltpu.VMEM((rounds, rows, cols), bf16),
            pltpu.VMEM((rounds, rows, cols), bf16),
            pltpu.VMEM((rows, cols), bf16),
            dma((4, chunks // load_group)),
            dma((replicas - 1,)),
            dma((replicas - 1,)),
            dma((rounds,)),
            dma((rounds, chunks)),
            dma((2, hops)),
            dma((2, hops, chunks)),
            *(folding if spares else ()),
        ],
        compiler_params=pltpu.CompilerParams(
            collective_id=0, has_side_effects=True, vmem_limit_bytes=48 * 1024 * 1024
        ),
    )(*large, push_weight)


def solution(mesh):
    return jax.shard_map(
        per_device,
        mesh=mesh,
        in_specs=(
            P("replica", "shard", None),
            P("replica", "shard", None),
            P("replica", "shard", None),
            P(None, "replica", "shard", None),
            P("replica"),
        ),
        out_specs=P("replica", None, None),
        check_vma=False,
    )
```

```python
import functools

import jax
import jax.numpy as jnp
from jax import lax
from jax.experimental import pallas as pl
from jax.experimental.pallas import tpu as pltpu
from jax.sharding import PartitionSpec as P

STEPS = 4


beta_one = 0.9
beta_two = 0.95
learn_rate = 0.1
decay_rate = 0.1
epsilon = 1e-08
adam_offset = 101

CODE_SCALE = 8.0
GAP_SCALE = 16.0
LAG = 3
HOP_LAG = 2
CHUNKS = 28
OPEN_LAG = 18
FOLD_LAG = 3
FULL_TAIL = 3
EAGER = 14
EARLY = 2
LOAD_GROUP = 2
SUB = 2
MESH = pl.DeviceIdType.MESH


def plan_of(replicas):
    levels = replicas.bit_length() - 1
    distances = [2 ** (step % levels) for step in range(STEPS)]
    every = {2**level for level in range(levels)}
    plan = []
    for step, distance in enumerate(distances):
        later = set(distances[step + 1 :])
        if every <= later:
            continue
        above = {d for d in every if d > distance}
        plan.append((step, distance, above <= later))
    return plan


def mixes_of(replicas):
    levels = replicas.bit_length() - 1
    mixes = [{0: 1.0}]
    for step in range(STEPS):
        distance, mixed = 2 ** (step % levels), {}
        for k, share in mixes[-1].items():
            for back in (k, (k + distance) % replicas):
                mixed[back] = mixed.get(back, 0.0) + 0.5 * share
        mixes.append(mixed)
    return mixes


def encode(value, scale=CODE_SCALE):
    power = value * scale
    power = power * power
    power = power * power
    power = power * power
    power = power * power
    return jnp.where(value < 0.0, -power, power).astype(jnp.bfloat16)


def decode(code, scale=CODE_SCALE):
    code = code.astype(jnp.float32)
    size = jnp.exp(jnp.log(jnp.abs(code)) * (1.0 / 16.0)) * (1.0 / scale)
    return jnp.where(code < 0.0, -size, size)


def kernel(
    plan, mixes, replicas, shards, chunks, chunk, sub, load_group, spares,
    params_ref, first_ref, second_ref, grads_ref, weight_ref, out_ref,
    params, first, second, grads, weights, scales, acc, terms, early, sent, arrived, final,
    load_sem, wsend, wrecv, xsend, xrecv, zsend, zrecv,
    codes=None, extra=None, hold=None, gap=None, gaps=None,
    rsend=None, rrecv=None, gsend=None, grecv=None,
):
    me, z = lax.axis_index("replica"), lax.axis_index("shard")
    rows = params.shape[0]
    rounds = len(plan)
    ends = [step for step, _, _ in plan]
    keep = 1.0 - learn_rate * decay_rate
    coded = spares > 0
    side, column, line = lax.rem(me, 2), lax.rem(me // 2, 2), me // 4
    foreign = shards - 1

    def columns(i):
        return pl.ds(pl.multiple_of(i * chunk, chunk), chunk)

    def spread(count):
        return pl.ds(0, count * chunk)

    def at_end(z):
        return jnp.logical_or(z == 0, z == shards - 1)

    def spared(i):
        return jnp.logical_and(i >= 1, i <= 4 * spares)

    def same_column(i):
        return lax.rem(i - 1, 2) == column

    def same_line(i):
        return lax.rem((i - 1) // 2, 2) == line

    def folded_here(i):
        return lax.rem((i - 1) // 4, 2) == side

    def everything(*tests):
        return functools.reduce(jnp.logical_and, tests)

    def lacking(i):
        return everything(spared(i), folded_here(i), same_column(i), same_line(i))

    def slab(index):
        return pl.ds(pl.multiple_of(index * rows, rows), rows)

    def peer(offset):
        return lax.rem(me + offset + replicas, replicas)

    barrier = pltpu.get_barrier_semaphore()
    for k in range(1, replicas):
        pl.semaphore_signal(barrier, inc=1, device_id={"replica": peer(k)}, device_id_type=MESH)

    @pl.when(z > 0)
    def _():
        pl.semaphore_signal(barrier, inc=1, device_id={"shard": z - 1}, device_id_type=MESH)

    @pl.when(z < shards - 1)
    def _():
        pl.semaphore_signal(barrier, inc=1, device_id={"shard": z + 1}, device_id_type=MESH)

    def loads(g):
        cols = pl.ds(pl.multiple_of(g * (load_group * chunk), chunk), load_group * chunk)
        return (
            pltpu.make_async_copy(params_ref.at[0, :, cols], params.at[:, cols], load_sem.at[0, g]),
            pltpu.make_async_copy(first_ref.at[0, :, cols], first.at[:, cols], load_sem.at[1, g]),
            pltpu.make_async_copy(second_ref.at[0, :, cols], second.at[:, cols], load_sem.at[2, g]),
            pltpu.make_async_copy(grads_ref.at[:, 0, :, cols], grads.at[:, :, cols], load_sem.at[3, g]),
        )

    @pl.loop(0, chunks // load_group)
    def _(g):
        for copy in loads(g):
            copy.start()

    weights[me] = jnp.full(weights.shape[1:], weight_ref[0], jnp.float32)
    ends_of_line = jnp.where(z > 0, 1, 0) + jnp.where(z < shards - 1, 1, 0)
    pl.semaphore_wait(barrier, replicas - 1 + ends_of_line)

    def weight_copy(k, owner):
        return pltpu.make_async_remote_copy(
            src_ref=weights.at[owner], dst_ref=weights.at[owner],
            send_sem=wsend.at[k - 1], recv_sem=wrecv.at[k - 1],
            device_id={"replica": peer(k)}, device_id_type=MESH,
        )

    for k in range(1, replicas):
        weight_copy(k, me).start()

    def wide(tile):
        tile = jnp.concatenate([tile] * (rows // tile.shape[0]), axis=0) if rows > tile.shape[0] else tile[:rows]
        return jnp.concatenate([tile] * (sub // tile.shape[1]), axis=1)

    heard = set()

    def mixed(level):
        total = None
        for k, share in sorted(mixes[level].items()):
            if k and k not in heard:
                weight_copy(k, peer(-k)).wait_recv()
                heard.add(k)
            part = share * weights[peer(-k)]
            total = part if total is None else total + part
        return total

    def scale_of(step):
        end = min(e for e in ends if e >= step)
        scales[1 + step] = wide(mixed(step) * (learn_rate * keep ** (end - step)))

    def exchange(k, i):
        _, distance, swap = plan[k]
        if swap:
            to = me + distance - 2 * distance * lax.rem(me // distance, 2)
        else:
            to = peer(distance)
        cols = slice(None) if i is None else columns(i)
        return pltpu.make_async_remote_copy(
            src_ref=sent.at[k, :, cols], dst_ref=arrived.at[k, :, cols],
            send_sem=xsend.at[k], recv_sem=xrecv.at[k, 0 if i is None else i],
            device_id={"replica": to}, device_id_type=MESH,
        )

    def ring(index, cols):
        return codes.at[slab(index), cols] if coded else out_ref.at[0, slab(index), cols]

    def gather(way, hop, i, count=None):
        sign = 1 - 2 * way
        cols, index = columns(i) if count is None else spread(count), z - sign * hop
        target = ring(index, cols)
        return pltpu.make_async_remote_copy(
            src_ref=final.at[:, cols] if hop == 0 else target, dst_ref=target,
            send_sem=zsend.at[way, hop], recv_sem=zrecv.at[way, hop, i],
            device_id={"shard": z + sign}, device_id_type=MESH,
        )

    def gathered(way, hop, i):
        sign = 1 - 2 * way
        target = ring(z - sign * hop, columns(i))
        return pltpu.make_async_remote_copy(
            src_ref=target, dst_ref=target,
            send_sem=zsend.at[way, hop - 1], recv_sem=zrecv.at[way, hop - 1, i],
            device_id={"shard": z - sign}, device_id_type=MESH,
        )

    def outward(way):
        return z == shards - 2 if way == 0 else z == 1

    def eager(way, i):
        return jnp.logical_or(i < EAGER, jnp.logical_not(outward(way))) if coded else i >= 0

    def sends(way, hop, i):
        holds = jnp.logical_and(has_target(way), has_source(way, hop))
        if coded:
            holds = jnp.logical_and(holds, jnp.logical_not(jnp.logical_and(outward(way), lacking(i))))
        return holds

    def has_source(way, hop):
        return z >= hop if way == 0 else z + hop < shards

    def has_target(way):
        return z < shards - 1 if way == 0 else z > 0

    def adam(cols, known):
        m, v = first[:, cols], second[:, cols]
        total = scales[0] * params[:, cols]
        for step in range(STEPS):
            g = grads[step, :, cols].astype(jnp.float32)
            count = adam_offset + step
            m = beta_one * m + (1.0 - beta_one) * g
            v = beta_two * v + (1.0 - beta_two) * g * g
            fixed = jnp.sqrt(v * (1.0 / (1.0 - beta_two**count))) + epsilon
            update = m * (1.0 / (1.0 - beta_one**count)) / fixed
            if step > ends[0]:
                terms[step - ends[0] - 1, :, cols] = update
            elif step < known:
                total = total - update * scales[1 + step]
            else:
                early[step - known, :, cols] = update
        return total

    def tiles(i):
        for j in range(chunk // sub):
            yield pl.ds(pl.multiple_of(i * chunk + j * sub, sub), sub)

    def first_half(i):
        for cols in tiles(i):
            acc[:, cols] = adam(cols, 1)

    def second_half(i):
        for cols in tiles(i):
            total = acc[:, cols]
            for step in range(1, ends[0] + 1):
                total = total - early[step - 1, :, cols] * scales[1 + step]
            acc[:, cols] = total
            sent[0, :, cols] = encode(total)
        exchange(0, i).start()

    def start_round(i):
        for cols in tiles(i):
            total = adam(cols, STEPS)
            acc[:, cols] = total
            sent[0, :, cols] = encode(total)
        exchange(0, i).start()

    def next_round(k, i):
        exchange(k - 1, i).wait_recv()
        for cols in tiles(i):
            both = acc[:, cols] + decode(arrived[k - 1, :, cols])
            if k < rounds:
                both = both * (0.5 * keep ** (ends[k] - ends[k - 1])) - terms[k - 1, :, cols] * scales[1 + ends[k]]
                acc[:, cols] = both
                sent[k, :, cols] = encode(both)
            else:
                done = (both * scales[1 + STEPS]).astype(jnp.bfloat16)
                out_ref[0, slab(z), cols] = done
                final[:, cols] = encode(0.5 * both) if coded else done
        if k < rounds:
            exchange(k, i).start()
        else:
            for way in range(2):
                pl.when(everything(sends(way, 0, i), eager(way, i)))(lambda way=way: gather(way, 0, i).start())

    def pass_on(hop, i):
        for way in range(2):

            @pl.when(everything(has_target(way), has_source(way, hop), eager(way, i)))
            def _(way=way):
                gathered(way, hop, i).wait_recv()

            @pl.when(everything(sends(way, hop, i), eager(way, i)))
            def _(way=way):
                gather(way, hop, i).start()

    def send_out(i):
        for way in range(2):

            @pl.when(everything(has_target(way), outward(way), i >= EAGER))
            def _(way=way):
                pl.when(sends(way, 0, i))(lambda: gather(way, 0, i).start())
                for hop in range(1, shards - 1):

                    @pl.when(has_source(way, hop))
                    def _(hop=hop):
                        gathered(way, hop, i).wait_recv()
                        pl.when(sends(way, hop, i))(lambda: gather(way, hop, i).start())

    def collect(i):
        for way in range(2):

            @pl.when(jnp.logical_not(has_target(way)))
            def _(way=way):
                for hop in range(1, shards):
                    gathered(way, hop, i).wait_recv()

    def abroad(j):
        return slab(j + jnp.where(j >= z, 1, 0))

    def relay(i, count=None):
        cols = columns(i) if count is None else spread(count)
        start = jnp.where(z == 0, rows, 0)
        return pltpu.make_async_remote_copy(
            src_ref=codes.at[pl.ds(pl.multiple_of(start, rows), foreign * rows), cols], dst_ref=extra.at[:, cols],
            send_sem=rsend, recv_sem=rrecv.at[i],
            device_id={"replica": me + 1 - 2 * side}, device_id_type=MESH,
        )

    def share(hop, i, count=None):
        cols = columns(i) if count is None else spread(count)
        to = me + 2 - 4 * column if hop else me + 4 - 8 * line
        return pltpu.make_async_remote_copy(
            src_ref=gap.at[:, cols], dst_ref=gaps.at[hop, :, cols],
            send_sem=gsend.at[hop], recv_sem=grecv.at[hop, i],
            device_id={"replica": to}, device_id_type=MESH,
        )

    def foreign_tiles(i):
        for j in range(foreign):
            for cols, held in zip(tiles(i), tiles(lax.rem(i, 8))):
                yield pl.ds(j * rows, rows), abroad(j), cols, held

    def put(where, cols, value):
        out_ref[0, where, cols] = (value * scales[2 + STEPS]).astype(jnp.bfloat16)

    def open_slabs(i):
        folds = jnp.logical_and(at_end(z), spared(i))

        @pl.when(jnp.logical_and(at_end(z), jnp.logical_not(lacking(i))))
        def _():
            collect(i)

        @pl.when(jnp.logical_and(folds, jnp.logical_not(folded_here(i))))
        def _():
            relay(i).start()

        @pl.when(jnp.logical_not(jnp.logical_and(folds, folded_here(i))))
        def _():
            for _, where, cols, _ in foreign_tiles(i):
                put(where, cols, decode(codes[where, cols]))

    def begin_fold(i):
        @pl.when(everything(at_end(z), spared(i), folded_here(i), jnp.logical_not(lacking(i))))
        def _():
            relay(i).wait_recv()
            for at, where, cols, held in foreign_tiles(i):
                value = decode(codes[where, cols])
                put(where, cols, value)
                apart = decode(extra[at, cols]) - value
                hold[at, held] = apart
                gap[at, cols] = encode(apart, GAP_SCALE)

            @pl.when(jnp.logical_not(same_line(i)))
            def _():
                share(0, i).start()

    def join_fold(i):
        @pl.when(everything(at_end(z), spared(i), folded_here(i), same_line(i), jnp.logical_not(same_column(i))))
        def _():
            share(0, i).wait_recv()
            for at, _, cols, held in foreign_tiles(i):
                gap[at, cols] = encode(hold[at, held] + decode(gaps[0, at, cols], GAP_SCALE), GAP_SCALE)
            share(1, i).start()

    def end_fold(i):
        @pl.when(jnp.logical_and(at_end(z), lacking(i)))
        def _():
            relay(i).wait_recv()
            share(0, i).wait_recv()
            share(1, i).wait_recv()
            for at, where, cols, _ in foreign_tiles(i):
                apart = decode(gaps[0, at, cols], GAP_SCALE) + decode(gaps[1, at, cols], GAP_SCALE)
                put(where, cols, decode(extra[at, cols]) + apart)

    def wait_loads(i):
        @pl.when(lax.rem(i, load_group) == 0)
        def _():
            for copy in loads(i // load_group):
                copy.wait()

    scales[0] = wide(mixed(0) * keep ** (ends[0] + 1))
    scale_of(0)
    for i in range(EARLY):
        if i % load_group == 0:
            for copy in loads(i // load_group):
                copy.wait()
        first_half(i)
    for step in range(1, ends[0] + 1):
        scale_of(step)
    for i in range(EARLY):
        second_half(i)
    wait_loads(EARLY)
    start_round(EARLY)
    for step in range(ends[0] + 1, STEPS):
        scale_of(step)
    scales[1 + STEPS] = wide(0.5 / mixed(STEPS))
    scales[2 + STEPS] = wide(1.0 / mixed(STEPS))

    def catch_up(slot, final_slot, delay, act):
        until = jnp.where(slot == final_slot, 4 * spares + 1, slot - delay)

        @pl.when(jnp.logical_and(slot > delay, slot <= final_slot))
        def _():
            @pl.loop(slot - 1 - delay, until)
            def _(i):
                act(i)

    hops = max(shards - 2, 0)
    last = rounds * LAG
    late = max(last + hops * HOP_LAG, OPEN_LAG)

    @pl.loop(EARLY + 1, chunks + (late + 1 if coded else last + hops * HOP_LAG))
    def _(t):
        def at(delay, act):
            i = t - delay

            @pl.when(jnp.logical_and(i >= 0, i < chunks))
            def _():
                act(i)

        @pl.when(t < chunks)
        def _():
            wait_loads(t)
            start_round(t)

        for k in range(1, rounds + 1):
            at(k * LAG, functools.partial(next_round, k))
        for hop in range(1, hops + 1):
            at(last + hop * HOP_LAG, functools.partial(pass_on, hop))
        if coded:
            at(last + hops * HOP_LAG, send_out)
            at(late + 1, begin_fold)
            catch_up(t - late, chunks - 1, FOLD_LAG, join_fold)
            catch_up(t - late, chunks, 2 * FOLD_LAG, end_fold)
            at(late, open_slabs)

    if not coded:

        @pl.loop(0, chunks)
        def _(i):
            collect(i)

    for k in range(1, replicas):
        weight_copy(k, me).wait_send()
    for k in range(rounds):
        exchange(k, None).wait_send()
    for way in range(2):
        for hop in range(shards - 1):
            holds = jnp.logical_and(has_target(way), has_source(way, hop))
            if coded:
                less = outward(way)

                @pl.when(jnp.logical_and(holds, less))
                def _(way=way, hop=hop):
                    gather(way, hop, 0, chunks - spares // 2).wait_send()

                holds = jnp.logical_and(holds, jnp.logical_not(less))

            @pl.when(holds)
            def _(way=way, hop=hop):
                gather(way, hop, 0, chunks).wait_send()

    if coded:

        @pl.when(at_end(z))
        def _():
            relay(0, 2 * spares).wait_send()
            share(0, 0, spares).wait_send()
            share(1, 0, spares // 2).wait_send()


def per_device(params, first_moment, second_moment, grads, push_weight):
    replicas, shards = lax.axis_size("replica"), lax.axis_size("shard")
    _, rows, cols = params.shape
    units = cols // 128
    chunks = max(n for n in range(1, CHUNKS + 1) if units % n == 0)
    chunk = cols // chunks
    sub = max(128 * n for n in range(1, SUB + 1) if chunk % (128 * n) == 0)
    load_group = LOAD_GROUP if chunks % LOAD_GROUP == 0 else 1
    plan, mixes = plan_of(replicas), mixes_of(replicas)
    rounds = len(plan)
    alternate = replicas == 8 and plan[-1][1] == 1 and not plan[-1][2] and shards > 2
    spares = max(chunks - 1 - FULL_TAIL, 0) // 8 * 2 if alternate else 0
    f32, bf16, dma = jnp.float32, jnp.bfloat16, pltpu.SemaphoreType.DMA
    anywhere = pl.BlockSpec(memory_space=pl.ANY)
    body = functools.partial(kernel, plan, mixes, replicas, shards, chunks, chunk, sub, load_group, spares)
    hops = max(shards - 1, 1)
    large = (params, first_moment, second_moment, grads)
    large = tuple(pltpu.with_memory_space_constraint(x, pltpu.HBM) for x in large)
    apart = (shards - 1) * rows
    folding = (
        pltpu.VMEM((shards * rows, cols), bf16),
        pltpu.VMEM((apart, cols), bf16),
        pltpu.VMEM((apart, 8 * chunk), f32),
        pltpu.VMEM((apart, cols), bf16),
        pltpu.VMEM((2, apart, cols), bf16),
        dma,
        dma((chunks,)),
        dma((2,)),
        dma((2, chunks)),
    )
    return pl.pallas_call(
        body,
        out_shape=jax.ShapeDtypeStruct((1, rows * shards, cols), bf16),
        in_specs=[anywhere] * 4 + [pl.BlockSpec(memory_space=pltpu.SMEM)],
        out_specs=pl.BlockSpec(memory_space=pltpu.VMEM),
        scratch_shapes=[
            pltpu.VMEM((rows, cols), f32),
            pltpu.VMEM((rows, cols), f32),
            pltpu.VMEM((rows, cols), f32),
            pltpu.VMEM((STEPS, rows, cols), bf16),
            pltpu.VMEM((replicas, 8, 128), f32),
            pltpu.VMEM((STEPS + 3, rows, sub), f32),
            pltpu.VMEM((rows, cols), f32),
            pltpu.VMEM((max(rounds - 1, 1), rows, cols), f32),
            pltpu.VMEM((max(plan[0][0], 1), rows, EARLY * chunk), f32),
            pltpu.VMEM((rounds, rows, cols), bf16),
            pltpu.VMEM((rounds, rows, cols), bf16),
            pltpu.VMEM((rows, cols), bf16),
            dma((4, chunks // load_group)),
            dma((replicas - 1,)),
            dma((replicas - 1,)),
            dma((rounds,)),
            dma((rounds, chunks)),
            dma((2, hops)),
            dma((2, hops, chunks)),
            *(folding if spares else ()),
        ],
        compiler_params=pltpu.CompilerParams(
            collective_id=0, has_side_effects=True, vmem_limit_bytes=48 * 1024 * 1024
        ),
    )(*large, push_weight)


def solution(mesh):
    return jax.shard_map(
        per_device,
        mesh=mesh,
        in_specs=(
            P("replica", "shard", None),
            P("replica", "shard", None),
            P("replica", "shard", None),
            P(None, "replica", "shard", None),
            P("replica"),
        ),
        out_specs=P("replica", None, None),
        check_vma=False,
    )
```

```python
import functools

import jax
import jax.numpy as jnp
from jax import lax
from jax.experimental import pallas as pl
from jax.experimental.pallas import tpu as pltpu
from jax.sharding import PartitionSpec as P

STEPS = 4


beta_one = 0.9
beta_two = 0.95
learn_rate = 0.1
decay_rate = 0.1
epsilon = 1e-08
adam_offset = 101

CODE_SCALE = 8.0
GAP_SCALE = 16.0
LAG = 3
HOP_LAG = 3
NEXT_HOP_LAG = 3
CHUNKS = 28
OPEN_LAG = 20
FOLD_LAG = 3
SWIFT = 1
SWIFT_AT = 17
SWIFT_LAG = 3
FULL_TAIL = 3
EAGER = 14
EARLY = 2
LOAD_GROUP = 2
SUB = 2
MESH = pl.DeviceIdType.MESH


def plan_of(replicas):
    levels = replicas.bit_length() - 1
    distances = [2 ** (step % levels) for step in range(STEPS)]
    every = {2**level for level in range(levels)}
    plan = []
    for step, distance in enumerate(distances):
        later = set(distances[step + 1 :])
        if every <= later:
            continue
        above = {d for d in every if d > distance}
        plan.append((step, distance, above <= later))
    return plan


def mixes_of(replicas):
    levels = replicas.bit_length() - 1
    mixes = [{0: 1.0}]
    for step in range(STEPS):
        distance, mixed = 2 ** (step % levels), {}
        for k, share in mixes[-1].items():
            for back in (k, (k + distance) % replicas):
                mixed[back] = mixed.get(back, 0.0) + 0.5 * share
        mixes.append(mixed)
    return mixes


def hop_lag(hop):
    return HOP_LAG + (hop - 1) * NEXT_HOP_LAG if hop else 0


def encode(value, scale=CODE_SCALE):
    power = value * scale
    power = power * power
    power = power * power
    power = power * power
    power = power * power
    return jnp.where(value < 0.0, -power, power).astype(jnp.bfloat16)


def decode(code, scale=CODE_SCALE):
    code = code.astype(jnp.float32)
    size = jnp.exp(jnp.log(jnp.abs(code)) * (1.0 / 16.0)) * (1.0 / scale)
    return jnp.where(code < 0.0, -size, size)


def kernel(
    plan, mixes, replicas, shards, chunks, chunk, sub, load_group, spares,
    params_ref, first_ref, second_ref, grads_ref, weight_ref, out_ref,
    params, first, second, grads, weights, scales, acc, terms, early, sent, arrived, final,
    load_sem, wsend, wrecv, xsend, xrecv, zsend, zrecv,
    codes=None, extra=None, hold=None, gap=None, gaps=None,
    beside=None,
    rsend=None, rrecv=None, gsend=None, grecv=None, bsend=None, brecv=None,
):
    me, z = lax.axis_index("replica"), lax.axis_index("shard")
    rows = params.shape[0]
    rounds = len(plan)
    ends = [step for step, _, _ in plan]
    keep = 1.0 - learn_rate * decay_rate
    coded = spares > 0
    swift = SWIFT if coded else 0
    side, column, line = lax.rem(me, 2), lax.rem(me // 2, 2), me // 4
    foreign = shards - 1

    def columns(i):
        return pl.ds(pl.multiple_of(i * chunk, chunk), chunk)

    def spread(count):
        return pl.ds(0, count * chunk)

    def at_end(z):
        return jnp.logical_or(z == 0, z == shards - 1)

    def spared(i):
        return jnp.logical_and(i >= swift, i < swift + 4 * spares)

    def same_column(i):
        return lax.rem(i - swift, 2) == column

    def same_line(i):
        return lax.rem((i - swift) // 2, 2) == line

    def folded_here(i):
        return lax.rem((i - swift) // 4, 2) == side

    def everything(*tests):
        return functools.reduce(jnp.logical_and, tests)

    def lacking(i):
        return everything(spared(i), folded_here(i), same_column(i), same_line(i))

    def slab(index):
        return pl.ds(pl.multiple_of(index * rows, rows), rows)

    def peer(offset):
        return lax.rem(me + offset + replicas, replicas)

    barrier = pltpu.get_barrier_semaphore()
    for k in range(1, replicas):
        pl.semaphore_signal(barrier, inc=1, device_id={"replica": peer(k)}, device_id_type=MESH)

    @pl.when(z > 0)
    def _():
        pl.semaphore_signal(barrier, inc=1, device_id={"shard": z - 1}, device_id_type=MESH)

    @pl.when(z < shards - 1)
    def _():
        pl.semaphore_signal(barrier, inc=1, device_id={"shard": z + 1}, device_id_type=MESH)

    def loads(g):
        cols = pl.ds(pl.multiple_of(g * (load_group * chunk), chunk), load_group * chunk)
        return (
            pltpu.make_async_copy(params_ref.at[0, :, cols], params.at[:, cols], load_sem.at[0, g]),
            pltpu.make_async_copy(first_ref.at[0, :, cols], first.at[:, cols], load_sem.at[1, g]),
            pltpu.make_async_copy(second_ref.at[0, :, cols], second.at[:, cols], load_sem.at[2, g]),
            pltpu.make_async_copy(grads_ref.at[:, 0, :, cols], grads.at[:, :, cols], load_sem.at[3, g]),
        )

    @pl.loop(0, chunks // load_group)
    def _(g):
        for copy in loads(g):
            copy.start()

    weights[me] = jnp.full(weights.shape[1:], weight_ref[0], jnp.float32)
    ends_of_line = jnp.where(z > 0, 1, 0) + jnp.where(z < shards - 1, 1, 0)
    pl.semaphore_wait(barrier, replicas - 1 + ends_of_line)

    def weight_copy(k, owner):
        return pltpu.make_async_remote_copy(
            src_ref=weights.at[owner], dst_ref=weights.at[owner],
            send_sem=wsend.at[k - 1], recv_sem=wrecv.at[k - 1],
            device_id={"replica": peer(k)}, device_id_type=MESH,
        )

    for k in range(1, replicas):
        weight_copy(k, me).start()

    def wide(tile):
        tile = jnp.concatenate([tile] * (rows // tile.shape[0]), axis=0) if rows > tile.shape[0] else tile[:rows]
        return jnp.concatenate([tile] * (sub // tile.shape[1]), axis=1)

    heard = set()

    def mixed(level):
        total = None
        for k, share in sorted(mixes[level].items()):
            if k and k not in heard:
                weight_copy(k, peer(-k)).wait_recv()
                heard.add(k)
            part = share * weights[peer(-k)]
            total = part if total is None else total + part
        return total

    def scale_of(step):
        end = min(e for e in ends if e >= step)
        scales[1 + step] = wide(mixed(step) * (learn_rate * keep ** (end - step)))

    def exchange(k, i):
        _, distance, swap = plan[k]
        if swap:
            to = me + distance - 2 * distance * lax.rem(me // distance, 2)
        else:
            to = peer(distance)
        cols = slice(None) if i is None else columns(i)
        return pltpu.make_async_remote_copy(
            src_ref=sent.at[k, :, cols], dst_ref=arrived.at[k, :, cols],
            send_sem=xsend.at[k], recv_sem=xrecv.at[k, 0 if i is None else i],
            device_id={"replica": to}, device_id_type=MESH,
        )

    def ring(index, cols):
        return codes.at[slab(index), cols] if coded else out_ref.at[0, slab(index), cols]

    def gather(way, hop, i, count=None, early=False):
        sign = 1 - 2 * way
        cols, index = columns(i) if count is None else spread(count), z - sign * hop
        target = ring(index, cols)
        return pltpu.make_async_remote_copy(
            src_ref=target if hop else sent.at[rounds - 1, :, cols] if early else final.at[:, cols], dst_ref=target,
            send_sem=zsend.at[way, hop], recv_sem=zrecv.at[way, hop, i],
            device_id={"shard": z + sign}, device_id_type=MESH,
        )

    def gathered(way, hop, i):
        sign = 1 - 2 * way
        target = ring(z - sign * hop, columns(i))
        return pltpu.make_async_remote_copy(
            src_ref=target, dst_ref=target,
            send_sem=zsend.at[way, hop - 1], recv_sem=zrecv.at[way, hop - 1, i],
            device_id={"shard": z - sign}, device_id_type=MESH,
        )

    def outward(way):
        return z == shards - 2 if way == 0 else z == 1

    def eager(way, i):
        return jnp.logical_or(i < EAGER, jnp.logical_not(outward(way))) if coded else i >= 0

    def sends(way, hop, i):
        holds = jnp.logical_and(has_target(way), has_source(way, hop))
        if coded:
            holds = jnp.logical_and(holds, jnp.logical_not(jnp.logical_and(outward(way), lacking(i))))
        return holds

    def has_source(way, hop):
        return z >= hop if way == 0 else z + hop < shards

    def has_target(way):
        return z < shards - 1 if way == 0 else z > 0

    def adam(cols, known):
        m, v = first[:, cols], second[:, cols]
        total = scales[0] * params[:, cols]
        for step in range(STEPS):
            g = grads[step, :, cols].astype(jnp.float32)
            count = adam_offset + step
            m = beta_one * m + (1.0 - beta_one) * g
            v = beta_two * v + (1.0 - beta_two) * g * g
            fixed = jnp.sqrt(v * (1.0 / (1.0 - beta_two**count))) + epsilon
            update = m * (1.0 / (1.0 - beta_one**count)) / fixed
            if step > ends[0]:
                terms[step - ends[0] - 1, :, cols] = update
            elif step < known:
                total = total - update * scales[1 + step]
            else:
                early[step - known, :, cols] = update
        return total

    def tiles(i):
        for j in range(chunk // sub):
            yield pl.ds(pl.multiple_of(i * chunk + j * sub, sub), sub)

    def first_half(i):
        for cols in tiles(i):
            acc[:, cols] = adam(cols, 1)

    def second_half(i):
        for cols in tiles(i):
            total = acc[:, cols]
            for step in range(1, ends[0] + 1):
                total = total - early[step - 1, :, cols] * scales[1 + step]
            acc[:, cols] = total
            sent[0, :, cols] = encode(total)
        exchange(0, i).start()

    def start_round(i):
        for cols in tiles(i):
            total = adam(cols, STEPS)
            acc[:, cols] = total
            sent[0, :, cols] = encode(total)
        exchange(0, i).start()

    def next_round(k, i):
        exchange(k - 1, i).wait_recv()
        for cols in tiles(i):
            both = acc[:, cols] + decode(arrived[k - 1, :, cols])
            if k < rounds:
                both = both * (0.5 * keep ** (ends[k] - ends[k - 1])) - terms[k - 1, :, cols] * scales[1 + ends[k]]
                acc[:, cols] = both
                sent[k, :, cols] = encode(both)
            else:
                done = (both * scales[1 + STEPS]).astype(jnp.bfloat16)
                out_ref[0, slab(z), cols] = done
                final[:, cols] = encode(0.5 * both) if coded else done
        if k < rounds:
            exchange(k, i).start()
            if k == rounds - 1 and swift:
                for way in range(2):
                    pl.when(jnp.logical_and(has_target(way), i < swift))(lambda way=way: gather(way, 0, i, early=True).start())
        else:
            for way in range(2):
                pl.when(everything(sends(way, 0, i), eager(way, i), i >= swift))(lambda way=way: gather(way, 0, i).start())

    def pass_on(hop, i):
        for way in range(2):

            @pl.when(everything(has_target(way), has_source(way, hop), eager(way, i)))
            def _(way=way):
                gathered(way, hop, i).wait_recv()

            @pl.when(everything(sends(way, hop, i), eager(way, i)))
            def _(way=way):
                gather(way, hop, i).start()

    def send_out(i):
        for way in range(2):

            @pl.when(everything(has_target(way), outward(way), i >= EAGER))
            def _(way=way):
                pl.when(sends(way, 0, i))(lambda: gather(way, 0, i).start())
                for hop in range(1, shards - 1):

                    @pl.when(has_source(way, hop))
                    def _(hop=hop):
                        gathered(way, hop, i).wait_recv()
                        pl.when(sends(way, hop, i))(lambda: gather(way, hop, i).start())

    def collect(i):
        for way in range(2):

            @pl.when(jnp.logical_not(has_target(way)))
            def _(way=way):
                for hop in range(1, shards):
                    gathered(way, hop, i).wait_recv()

    def abroad(j):
        return slab(j + jnp.where(j >= z, 1, 0))

    def relay(i, count=None):
        cols = columns(i) if count is None else spread(count)
        start = jnp.where(z == 0, rows, 0)
        return pltpu.make_async_remote_copy(
            src_ref=codes.at[pl.ds(pl.multiple_of(start, rows), foreign * rows), cols], dst_ref=extra.at[:, cols],
            send_sem=rsend, recv_sem=rrecv.at[i],
            device_id={"replica": me + 1 - 2 * side}, device_id_type=MESH,
        )

    def share(hop, i, count=None):
        cols = columns(i) if count is None else spread(count)
        to = me + 2 - 4 * column if hop else me + 4 - 8 * line
        return pltpu.make_async_remote_copy(
            src_ref=gap.at[:, cols], dst_ref=gaps.at[hop, :, cols],
            send_sem=gsend.at[hop], recv_sem=grecv.at[hop, i],
            device_id={"replica": to}, device_id_type=MESH,
        )

    def lend(i, j):
        return pltpu.make_async_remote_copy(
            src_ref=codes.at[abroad(j), columns(i)], dst_ref=beside.at[pl.ds(j * rows, rows), columns(i)],
            send_sem=bsend, recv_sem=brecv.at[i * foreign + j],
            device_id={"replica": peer(1)}, device_id_type=MESH,
        )

    def lend_swift(i):
        @pl.when(at_end(z))
        def _():
            collect(i)

        for j in range(foreign):
            lend(i, j).start()

    def open_swift(i):
        for j in range(foreign):
            lend(i, j).wait_recv()
        for at, where, cols, _ in foreign_tiles(i):
            both = decode(codes[where, cols]) + decode(beside[at, cols])
            out_ref[0, where, cols] = (both * scales[1 + STEPS]).astype(jnp.bfloat16)

    def foreign_tiles(i):
        for j in range(foreign):
            for cols, held in zip(tiles(i), tiles(lax.rem(i, 8))):
                yield pl.ds(j * rows, rows), abroad(j), cols, held

    def put(where, cols, value):
        out_ref[0, where, cols] = (value * scales[2 + STEPS]).astype(jnp.bfloat16)

    def open_slabs(i):
        folds = jnp.logical_and(at_end(z), spared(i))

        @pl.when(jnp.logical_and(at_end(z), jnp.logical_not(lacking(i))))
        def _():
            collect(i)

        @pl.when(jnp.logical_and(folds, jnp.logical_not(folded_here(i))))
        def _():
            relay(i).start()

        @pl.when(jnp.logical_not(jnp.logical_and(folds, folded_here(i))))
        def _():
            for _, where, cols, _ in foreign_tiles(i):
                put(where, cols, decode(codes[where, cols]))

    def begin_fold(i):
        @pl.when(everything(at_end(z), spared(i), folded_here(i), jnp.logical_not(lacking(i))))
        def _():
            relay(i).wait_recv()
            for at, where, cols, held in foreign_tiles(i):
                value = decode(codes[where, cols])
                put(where, cols, value)
                apart = decode(extra[at, cols]) - value
                hold[at, held] = apart
                gap[at, cols] = encode(apart, GAP_SCALE)

            @pl.when(jnp.logical_not(same_line(i)))
            def _():
                share(0, i).start()

    def join_fold(i):
        @pl.when(everything(at_end(z), spared(i), folded_here(i), same_line(i), jnp.logical_not(same_column(i))))
        def _():
            share(0, i).wait_recv()
            for at, _, cols, held in foreign_tiles(i):
                gap[at, cols] = encode(hold[at, held] + decode(gaps[0, at, cols], GAP_SCALE), GAP_SCALE)
            share(1, i).start()

    def end_fold(i):
        @pl.when(jnp.logical_and(at_end(z), lacking(i)))
        def _():
            relay(i).wait_recv()
            share(0, i).wait_recv()
            share(1, i).wait_recv()
            for at, where, cols, _ in foreign_tiles(i):
                apart = decode(gaps[0, at, cols], GAP_SCALE) + decode(gaps[1, at, cols], GAP_SCALE)
                put(where, cols, decode(extra[at, cols]) + apart)

    def wait_loads(i):
        @pl.when(lax.rem(i, load_group) == 0)
        def _():
            for copy in loads(i // load_group):
                copy.wait()

    scales[0] = wide(mixed(0) * keep ** (ends[0] + 1))
    scale_of(0)
    for i in range(EARLY):
        if i % load_group == 0:
            for copy in loads(i // load_group):
                copy.wait()
        first_half(i)
    for step in range(1, ends[0] + 1):
        scale_of(step)
    for i in range(EARLY):
        second_half(i)
    wait_loads(EARLY)
    start_round(EARLY)
    for step in range(ends[0] + 1, STEPS):
        scale_of(step)
    scales[1 + STEPS] = wide(0.5 / mixed(STEPS))
    scales[2 + STEPS] = wide(1.0 / mixed(STEPS))

    def catch_up(slot, final_slot, delay, act):
        until = jnp.where(slot == final_slot, 4 * spares + swift, slot - delay)

        @pl.when(jnp.logical_and(slot > delay, slot <= final_slot))
        def _():
            @pl.loop(slot - 1 - delay, until)
            def _(i):
                act(i)

    hops = max(shards - 2, 0)
    last = rounds * LAG
    late = max(last + hop_lag(hops), OPEN_LAG)

    @pl.loop(EARLY + 1, chunks + (late + 1 if coded else last + hop_lag(hops)))
    def _(t):
        def at(delay, act, low=0, high=chunks):
            i = t - delay

            @pl.when(jnp.logical_and(i >= low, i < high))
            def _():
                act(i)

        @pl.when(t < chunks)
        def _():
            wait_loads(t)
            start_round(t)

        for k in range(1, rounds + 1):
            at(k * LAG, functools.partial(next_round, k))
        for hop in range(1, hops + 1):
            at(last + hop_lag(hop), functools.partial(pass_on, hop), swift)
            if swift:
                at(last - LAG + hop_lag(hop), functools.partial(pass_on, hop), 0, swift)
        if coded:
            at(last + hop_lag(hops), send_out)
            at(late + 1, begin_fold)
            catch_up(t - late, chunks - 1, FOLD_LAG, join_fold)
            catch_up(t - late, chunks, 2 * FOLD_LAG, end_fold)
            at(late, open_slabs, swift)
            at(SWIFT_AT, lend_swift, 0, swift)
            at(SWIFT_AT + SWIFT_LAG, open_swift, 0, swift)

    if not coded:

        @pl.loop(0, chunks)
        def _(i):
            collect(i)

    for k in range(1, replicas):
        weight_copy(k, me).wait_send()
    for k in range(rounds):
        exchange(k, None).wait_send()
    for way in range(2):
        for hop in range(shards - 1):
            holds = jnp.logical_and(has_target(way), has_source(way, hop))
            if coded:
                less = outward(way)

                @pl.when(jnp.logical_and(holds, less))
                def _(way=way, hop=hop):
                    gather(way, hop, 0, chunks - spares // 2).wait_send()

                holds = jnp.logical_and(holds, jnp.logical_not(less))

            @pl.when(holds)
            def _(way=way, hop=hop):
                gather(way, hop, 0, chunks).wait_send()

    if coded:

        @pl.when(at_end(z))
        def _():
            relay(0, 2 * spares).wait_send()
            share(0, 0, spares).wait_send()
            share(1, 0, spares // 2).wait_send()

        pltpu.make_async_remote_copy(
            src_ref=beside, dst_ref=beside, send_sem=bsend, recv_sem=brecv.at[0],
            device_id={"replica": peer(1)}, device_id_type=MESH,
        ).wait_send()


def per_device(params, first_moment, second_moment, grads, push_weight):
    replicas, shards = lax.axis_size("replica"), lax.axis_size("shard")
    _, rows, cols = params.shape
    units = cols // 128
    chunks = max(n for n in range(1, CHUNKS + 1) if units % n == 0)
    chunk = cols // chunks
    sub = max(128 * n for n in range(1, SUB + 1) if chunk % (128 * n) == 0)
    load_group = LOAD_GROUP if chunks % LOAD_GROUP == 0 else 1
    plan, mixes = plan_of(replicas), mixes_of(replicas)
    rounds = len(plan)
    alternate = replicas == 8 and plan[-1][1] == 1 and not plan[-1][2] and shards > 2
    spares = max(chunks - SWIFT - FULL_TAIL, 0) // 8 * 2 if alternate else 0
    f32, bf16, dma = jnp.float32, jnp.bfloat16, pltpu.SemaphoreType.DMA
    anywhere = pl.BlockSpec(memory_space=pl.ANY)
    body = functools.partial(kernel, plan, mixes, replicas, shards, chunks, chunk, sub, load_group, spares)
    hops = max(shards - 1, 1)
    large = (params, first_moment, second_moment, grads)
    large = tuple(pltpu.with_memory_space_constraint(x, pltpu.HBM) for x in large)
    apart = (shards - 1) * rows
    folding = (
        pltpu.VMEM((shards * rows, cols), bf16),
        pltpu.VMEM((apart, cols), bf16),
        pltpu.VMEM((apart, 8 * chunk), f32),
        pltpu.VMEM((apart, cols), bf16),
        pltpu.VMEM((2, apart, cols), bf16),
        pltpu.VMEM((apart, SWIFT * chunk), bf16),
        dma,
        dma((chunks,)),
        dma((2,)),
        dma((2, chunks)),
        dma,
        dma((SWIFT * (shards - 1),)),
    )
    return pl.pallas_call(
        body,
        out_shape=jax.ShapeDtypeStruct((1, rows * shards, cols), bf16),
        in_specs=[anywhere] * 4 + [pl.BlockSpec(memory_space=pltpu.SMEM)],
        out_specs=pl.BlockSpec(memory_space=pltpu.VMEM),
        scratch_shapes=[
            pltpu.VMEM((rows, cols), f32),
            pltpu.VMEM((rows, cols), f32),
            pltpu.VMEM((rows, cols), f32),
            pltpu.VMEM((STEPS, rows, cols), bf16),
            pltpu.VMEM((replicas, 8, 128), f32),
            pltpu.VMEM((STEPS + 3, rows, sub), f32),
            pltpu.VMEM((rows, cols), f32),
            pltpu.VMEM((max(rounds - 1, 1), rows, cols), f32),
            pltpu.VMEM((max(plan[0][0], 1), rows, EARLY * chunk), f32),
            pltpu.VMEM((rounds, rows, cols), bf16),
            pltpu.VMEM((rounds, rows, cols), bf16),
            pltpu.VMEM((rows, cols), bf16),
            dma((4, chunks // load_group)),
            dma((replicas - 1,)),
            dma((replicas - 1,)),
            dma((rounds,)),
            dma((rounds, chunks)),
            dma((2, hops)),
            dma((2, hops, chunks)),
            *(folding if spares else ()),
        ],
        compiler_params=pltpu.CompilerParams(
            collective_id=0, has_side_effects=True, vmem_limit_bytes=48 * 1024 * 1024
        ),
    )(*large, push_weight)


def solution(mesh):
    return jax.shard_map(
        per_device,
        mesh=mesh,
        in_specs=(
            P("replica", "shard", None),
            P("replica", "shard", None),
            P("replica", "shard", None),
            P(None, "replica", "shard", None),
            P("replica"),
        ),
        out_specs=P("replica", None, None),
        check_vma=False,
    )
```

```python
import functools

import jax
import jax.numpy as jnp
from jax import lax
from jax.experimental import pallas as pl
from jax.experimental.pallas import tpu as pltpu
from jax.sharding import PartitionSpec as P

STEPS = 4


beta_one = 0.9
beta_two = 0.95
learn_rate = 0.1
decay_rate = 0.1
epsilon = 1e-08
adam_offset = 101

CODE_SCALE = 8.0
GAP_SCALE = 16.0
LAG = 3
HOP_LAG = 3
NEXT_HOP_LAG = 3
CHUNKS = 28
OPEN_LAG = 20
FOLD_LAG = 3
SWIFT = 1
SWIFT_AT = 17
SWIFT_LAG = 3
FULL_TAIL = 3
EAGER = 14
EARLY = 2
LOAD_GROUP = 4
SUB = 2
MESH = pl.DeviceIdType.MESH


def plan_of(replicas):
    levels = replicas.bit_length() - 1
    distances = [2 ** (step % levels) for step in range(STEPS)]
    every = {2**level for level in range(levels)}
    plan = []
    for step, distance in enumerate(distances):
        later = set(distances[step + 1 :])
        if every <= later:
            continue
        above = {d for d in every if d > distance}
        plan.append((step, distance, above <= later))
    return plan


def mixes_of(replicas):
    levels = replicas.bit_length() - 1
    mixes = [{0: 1.0}]
    for step in range(STEPS):
        distance, mixed = 2 ** (step % levels), {}
        for k, share in mixes[-1].items():
            for back in (k, (k + distance) % replicas):
                mixed[back] = mixed.get(back, 0.0) + 0.5 * share
        mixes.append(mixed)
    return mixes


def hop_lag(hop):
    return HOP_LAG + (hop - 1) * NEXT_HOP_LAG if hop else 0


def encode(value, scale=CODE_SCALE):
    power = value * scale
    power = power * power
    power = power * power
    power = power * power
    power = power * power
    return jnp.where(value < 0.0, -power, power).astype(jnp.bfloat16)


def decode(code, scale=CODE_SCALE):
    code = code.astype(jnp.float32)
    size = jnp.exp(jnp.log(jnp.abs(code)) * (1.0 / 16.0)) * (1.0 / scale)
    return jnp.where(code < 0.0, -size, size)


def kernel(
    plan, mixes, replicas, shards, chunks, chunk, sub, load_group, spares,
    params_ref, first_ref, second_ref, grads_ref, weight_ref, out_ref,
    params, first, second, grads, weights, scales, acc, terms, early, sent, arrived, final,
    load_sem, wsend, wrecv, xsend, xrecv, zsend, zrecv,
    codes=None, extra=None, hold=None, gap=None, gaps=None,
    beside=None,
    rsend=None, rrecv=None, gsend=None, grecv=None, bsend=None, brecv=None,
    lead=None, lsend=None, lrecv=None,
):
    me, z = lax.axis_index("replica"), lax.axis_index("shard")
    rows = params.shape[0]
    rounds = len(plan)
    ends = [step for step, _, _ in plan]
    keep = 1.0 - learn_rate * decay_rate
    coded = spares > 0
    swift = SWIFT if coded else 0
    leads = coded and ends[0] == 1 and plan[0][2]
    side, column, line = lax.rem(me, 2), lax.rem(me // 2, 2), me // 4
    foreign = shards - 1

    def columns(i):
        return pl.ds(pl.multiple_of(i * chunk, chunk), chunk)

    def spread(count):
        return pl.ds(0, count * chunk)

    def at_end(z):
        return jnp.logical_or(z == 0, z == shards - 1)

    def spared(i):
        return jnp.logical_and(i >= swift, i < swift + 4 * spares)

    def same_column(i):
        return lax.rem(i - swift, 2) == column

    def same_line(i):
        return lax.rem((i - swift) // 2, 2) == line

    def folded_here(i):
        return lax.rem((i - swift) // 4, 2) == side

    def everything(*tests):
        return functools.reduce(jnp.logical_and, tests)

    def lacking(i):
        return everything(spared(i), folded_here(i), same_column(i), same_line(i))

    def slab(index):
        return pl.ds(pl.multiple_of(index * rows, rows), rows)

    def peer(offset):
        return lax.rem(me + offset + replicas, replicas)

    barrier = pltpu.get_barrier_semaphore()
    for k in range(1, replicas):
        pl.semaphore_signal(barrier, inc=1, device_id={"replica": peer(k)}, device_id_type=MESH)

    @pl.when(z > 0)
    def _():
        pl.semaphore_signal(barrier, inc=1, device_id={"shard": z - 1}, device_id_type=MESH)

    @pl.when(z < shards - 1)
    def _():
        pl.semaphore_signal(barrier, inc=1, device_id={"shard": z + 1}, device_id_type=MESH)

    def loads(g):
        cols = pl.ds(pl.multiple_of(g * (load_group * chunk), chunk), load_group * chunk)
        return (
            pltpu.make_async_copy(params_ref.at[0, :, cols], params.at[:, cols], load_sem.at[0, g]),
            pltpu.make_async_copy(first_ref.at[0, :, cols], first.at[:, cols], load_sem.at[1, g]),
            pltpu.make_async_copy(second_ref.at[0, :, cols], second.at[:, cols], load_sem.at[2, g]),
            pltpu.make_async_copy(grads_ref.at[:, 0, :, cols], grads.at[:, :, cols], load_sem.at[3, g]),
        )

    @pl.loop(0, chunks // load_group)
    def _(g):
        for copy in loads(g):
            copy.start()

    weights[me] = jnp.full(weights.shape[1:], weight_ref[0], jnp.float32)
    ends_of_line = jnp.where(z > 0, 1, 0) + jnp.where(z < shards - 1, 1, 0)
    pl.semaphore_wait(barrier, replicas - 1 + ends_of_line)

    def weight_copy(k, owner):
        return pltpu.make_async_remote_copy(
            src_ref=weights.at[owner], dst_ref=weights.at[owner],
            send_sem=wsend.at[k - 1], recv_sem=wrecv.at[k - 1],
            device_id={"replica": peer(k)}, device_id_type=MESH,
        )

    for k in range(1, replicas):
        weight_copy(k, me).start()

    def wide(tile):
        tile = jnp.concatenate([tile] * (rows // tile.shape[0]), axis=0) if rows > tile.shape[0] else tile[:rows]
        return jnp.concatenate([tile] * (sub // tile.shape[1]), axis=1)

    heard = set()

    def mixed(level):
        total = None
        for k, share in sorted(mixes[level].items()):
            if k and k not in heard:
                weight_copy(k, peer(-k)).wait_recv()
                heard.add(k)
            part = share * weights[peer(-k)]
            total = part if total is None else total + part
        return total

    def scale_of(step):
        end = min(e for e in ends if e >= step)
        scales[1 + step] = wide(mixed(step) * (learn_rate * keep ** (end - step)))

    def partner(k):
        _, distance, swap = plan[k]
        return me + distance - 2 * distance * lax.rem(me // distance, 2) if swap else peer(distance)

    def lead_copy():
        return pltpu.make_async_remote_copy(
            src_ref=lead.at[0], dst_ref=lead.at[1], send_sem=lsend, recv_sem=lrecv,
            device_id={"replica": partner(0)}, device_id_type=MESH,
        )

    def start_early():
        for cols in tiles(0):
            sent[0, :, cols] = encode(acc[:, cols])
            lead[0, :, cols] = encode(early[0, :, cols])
        exchange(0, 0).start()
        lead_copy().start()

    def finish_early():
        lead_copy().wait_recv()
        for cols in tiles(0):
            acc[:, cols] = acc[:, cols] - decode(lead[1, :, cols]) * scales[3 + STEPS]

    def exchange(k, i):
        to = partner(k)
        cols = slice(None) if i is None else columns(i)
        return pltpu.make_async_remote_copy(
            src_ref=sent.at[k, :, cols], dst_ref=arrived.at[k, :, cols],
            send_sem=xsend.at[k], recv_sem=xrecv.at[k, 0 if i is None else i],
            device_id={"replica": to}, device_id_type=MESH,
        )

    def ring(index, cols):
        return codes.at[slab(index), cols] if coded else out_ref.at[0, slab(index), cols]

    def gather(way, hop, i, count=None, early=False):
        sign = 1 - 2 * way
        cols, index = columns(i) if count is None else spread(count), z - sign * hop
        target = ring(index, cols)
        return pltpu.make_async_remote_copy(
            src_ref=target if hop else sent.at[rounds - 1, :, cols] if early else final.at[:, cols], dst_ref=target,
            send_sem=zsend.at[way, hop], recv_sem=zrecv.at[way, hop, i],
            device_id={"shard": z + sign}, device_id_type=MESH,
        )

    def gathered(way, hop, i):
        sign = 1 - 2 * way
        target = ring(z - sign * hop, columns(i))
        return pltpu.make_async_remote_copy(
            src_ref=target, dst_ref=target,
            send_sem=zsend.at[way, hop - 1], recv_sem=zrecv.at[way, hop - 1, i],
            device_id={"shard": z - sign}, device_id_type=MESH,
        )

    def outward(way):
        return z == shards - 2 if way == 0 else z == 1

    def eager(way, i):
        return jnp.logical_or(i < EAGER, jnp.logical_not(outward(way))) if coded else i >= 0

    def sends(way, hop, i):
        holds = jnp.logical_and(has_target(way), has_source(way, hop))
        if coded:
            holds = jnp.logical_and(holds, jnp.logical_not(jnp.logical_and(outward(way), lacking(i))))
        return holds

    def has_source(way, hop):
        return z >= hop if way == 0 else z + hop < shards

    def has_target(way):
        return z < shards - 1 if way == 0 else z > 0

    def adam(cols, known):
        m, v = first[:, cols], second[:, cols]
        total = scales[0] * params[:, cols]
        for step in range(STEPS):
            g = grads[step, :, cols].astype(jnp.float32)
            count = adam_offset + step
            m = beta_one * m + (1.0 - beta_one) * g
            v = beta_two * v + (1.0 - beta_two) * g * g
            fixed = jnp.sqrt(v * (1.0 / (1.0 - beta_two**count))) + epsilon
            update = m * (1.0 / (1.0 - beta_one**count)) / fixed
            if step > ends[0]:
                terms[step - ends[0] - 1, :, cols] = update
            elif step < known:
                total = total - update * scales[1 + step]
            else:
                early[step - known, :, cols] = update
        return total

    def tiles(i):
        for j in range(chunk // sub):
            yield pl.ds(pl.multiple_of(i * chunk + j * sub, sub), sub)

    def first_half(i):
        for cols in tiles(i):
            acc[:, cols] = adam(cols, 1)

    def second_half(i):
        for cols in tiles(i):
            total = acc[:, cols]
            for step in range(1, ends[0] + 1):
                total = total - early[step - 1, :, cols] * scales[1 + step]
            acc[:, cols] = total
            if not (leads and i == 0):
                sent[0, :, cols] = encode(total)
        if not (leads and i == 0):
            exchange(0, i).start()

    def start_round(i):
        for cols in tiles(i):
            total = adam(cols, STEPS)
            acc[:, cols] = total
            sent[0, :, cols] = encode(total)
        exchange(0, i).start()

    def next_round(k, i):
        exchange(k - 1, i).wait_recv()
        if k == 1 and leads:
            pl.when(i == 0)(finish_early)
        for cols in tiles(i):
            both = acc[:, cols] + decode(arrived[k - 1, :, cols])
            if k < rounds:
                both = both * (0.5 * keep ** (ends[k] - ends[k - 1])) - terms[k - 1, :, cols] * scales[1 + ends[k]]
                acc[:, cols] = both
                sent[k, :, cols] = encode(both)
            else:
                done = (both * scales[1 + STEPS]).astype(jnp.bfloat16)
                out_ref[0, slab(z), cols] = done
                final[:, cols] = encode(0.5 * both) if coded else done
        if k < rounds:
            exchange(k, i).start()
            if k == rounds - 1 and swift:
                for way in range(2):
                    pl.when(jnp.logical_and(has_target(way), i < swift))(lambda way=way: gather(way, 0, i, early=True).start())
        else:
            for way in range(2):
                pl.when(everything(sends(way, 0, i), eager(way, i), i >= swift))(lambda way=way: gather(way, 0, i).start())

    def pass_on(hop, i):
        for way in range(2):

            @pl.when(everything(has_target(way), has_source(way, hop), eager(way, i)))
            def _(way=way):
                gathered(way, hop, i).wait_recv()

            @pl.when(everything(sends(way, hop, i), eager(way, i)))
            def _(way=way):
                gather(way, hop, i).start()

    def send_out(i):
        for way in range(2):

            @pl.when(everything(has_target(way), outward(way), i >= EAGER))
            def _(way=way):
                pl.when(sends(way, 0, i))(lambda: gather(way, 0, i).start())
                for hop in range(1, shards - 1):

                    @pl.when(has_source(way, hop))
                    def _(hop=hop):
                        gathered(way, hop, i).wait_recv()
                        pl.when(sends(way, hop, i))(lambda: gather(way, hop, i).start())

    def collect(i):
        for way in range(2):

            @pl.when(jnp.logical_not(has_target(way)))
            def _(way=way):
                for hop in range(1, shards):
                    gathered(way, hop, i).wait_recv()

    def abroad(j):
        return slab(j + jnp.where(j >= z, 1, 0))

    def relay(i, count=None):
        cols = columns(i) if count is None else spread(count)
        start = jnp.where(z == 0, rows, 0)
        return pltpu.make_async_remote_copy(
            src_ref=codes.at[pl.ds(pl.multiple_of(start, rows), foreign * rows), cols], dst_ref=extra.at[:, cols],
            send_sem=rsend, recv_sem=rrecv.at[i],
            device_id={"replica": me + 1 - 2 * side}, device_id_type=MESH,
        )

    def share(hop, i, count=None):
        cols = columns(i) if count is None else spread(count)
        to = me + 2 - 4 * column if hop else me + 4 - 8 * line
        return pltpu.make_async_remote_copy(
            src_ref=gap.at[:, cols], dst_ref=gaps.at[hop, :, cols],
            send_sem=gsend.at[hop], recv_sem=grecv.at[hop, i],
            device_id={"replica": to}, device_id_type=MESH,
        )

    def lend(i, j):
        return pltpu.make_async_remote_copy(
            src_ref=codes.at[abroad(j), columns(i)], dst_ref=beside.at[pl.ds(j * rows, rows), columns(i)],
            send_sem=bsend, recv_sem=brecv.at[i * foreign + j],
            device_id={"replica": peer(1)}, device_id_type=MESH,
        )

    def lend_swift(i):
        @pl.when(at_end(z))
        def _():
            collect(i)

        for j in range(foreign):
            lend(i, j).start()

    def open_swift(i):
        for j in range(foreign):
            lend(i, j).wait_recv()
        for at, where, cols, _ in foreign_tiles(i):
            both = decode(codes[where, cols]) + decode(beside[at, cols])
            out_ref[0, where, cols] = (both * scales[1 + STEPS]).astype(jnp.bfloat16)

    def foreign_tiles(i):
        for j in range(foreign):
            for cols, held in zip(tiles(i), tiles(lax.rem(i, 8))):
                yield pl.ds(j * rows, rows), abroad(j), cols, held

    def put(where, cols, value):
        out_ref[0, where, cols] = (value * scales[2 + STEPS]).astype(jnp.bfloat16)

    def open_slabs(i):
        folds = jnp.logical_and(at_end(z), spared(i))

        @pl.when(jnp.logical_and(at_end(z), jnp.logical_not(lacking(i))))
        def _():
            collect(i)

        @pl.when(jnp.logical_and(folds, jnp.logical_not(folded_here(i))))
        def _():
            relay(i).start()

        @pl.when(jnp.logical_not(jnp.logical_and(folds, folded_here(i))))
        def _():
            for _, where, cols, _ in foreign_tiles(i):
                put(where, cols, decode(codes[where, cols]))

    def begin_fold(i):
        @pl.when(everything(at_end(z), spared(i), folded_here(i), jnp.logical_not(lacking(i))))
        def _():
            relay(i).wait_recv()
            for at, where, cols, held in foreign_tiles(i):
                value = decode(codes[where, cols])
                put(where, cols, value)
                apart = decode(extra[at, cols]) - value
                hold[at, held] = apart
                gap[at, cols] = encode(apart, GAP_SCALE)

            @pl.when(jnp.logical_not(same_line(i)))
            def _():
                share(0, i).start()

    def join_fold(i):
        @pl.when(everything(at_end(z), spared(i), folded_here(i), same_line(i), jnp.logical_not(same_column(i))))
        def _():
            share(0, i).wait_recv()
            for at, _, cols, held in foreign_tiles(i):
                gap[at, cols] = encode(hold[at, held] + decode(gaps[0, at, cols], GAP_SCALE), GAP_SCALE)
            share(1, i).start()

    def end_fold(i):
        @pl.when(jnp.logical_and(at_end(z), lacking(i)))
        def _():
            relay(i).wait_recv()
            share(0, i).wait_recv()
            share(1, i).wait_recv()
            for at, where, cols, _ in foreign_tiles(i):
                apart = decode(gaps[0, at, cols], GAP_SCALE) + decode(gaps[1, at, cols], GAP_SCALE)
                put(where, cols, decode(extra[at, cols]) + apart)

    def wait_loads(i):
        @pl.when(lax.rem(i, load_group) == 0)
        def _():
            for copy in loads(i // load_group):
                copy.wait()

    scales[0] = wide(mixed(0) * keep ** (ends[0] + 1))
    scale_of(0)
    for i in range(EARLY):
        if i % load_group == 0:
            for copy in loads(i // load_group):
                copy.wait()
        first_half(i)
        if leads and i == 0:
            start_early()
    for step in range(1, ends[0] + 1):
        scale_of(step)
    for i in range(EARLY):
        second_half(i)
    wait_loads(EARLY)
    start_round(EARLY)
    for step in range(ends[0] + 1, STEPS):
        scale_of(step)
    scales[1 + STEPS] = wide(0.5 / mixed(STEPS))
    scales[2 + STEPS] = wide(1.0 / mixed(STEPS))
    if leads:
        theirs = sum(share * weights[lax.rem(partner(0) - k + replicas, replicas)] for k, share in mixes[1].items())
        scales[3 + STEPS] = wide(theirs * learn_rate)

    def catch_up(slot, final_slot, delay, act):
        until = jnp.where(slot == final_slot, 4 * spares + swift, slot - delay)

        @pl.when(jnp.logical_and(slot > delay, slot <= final_slot))
        def _():
            @pl.loop(slot - 1 - delay, until)
            def _(i):
                act(i)

    hops = max(shards - 2, 0)
    last = rounds * LAG
    late = max(last + hop_lag(hops), OPEN_LAG)

    @pl.loop(EARLY + 1, chunks + (late + 1 if coded else last + hop_lag(hops)))
    def _(t):
        def at(delay, act, low=0, high=chunks):
            i = t - delay

            @pl.when(jnp.logical_and(i >= low, i < high))
            def _():
                act(i)

        @pl.when(t < chunks)
        def _():
            wait_loads(t)
            start_round(t)

        for k in range(1, rounds + 1):
            at(k * LAG, functools.partial(next_round, k))
        for hop in range(1, hops + 1):
            at(last + hop_lag(hop), functools.partial(pass_on, hop), swift)
            if swift:
                at(last - LAG + hop_lag(hop), functools.partial(pass_on, hop), 0, swift)
        if coded:
            at(last + hop_lag(hops), send_out)
            at(late + 1, begin_fold)
            catch_up(t - late, chunks - 1, FOLD_LAG, join_fold)
            catch_up(t - late, chunks, 2 * FOLD_LAG, end_fold)
            at(late, open_slabs, swift)
            at(SWIFT_AT, lend_swift, 0, swift)
            at(SWIFT_AT + SWIFT_LAG, open_swift, 0, swift)

    if not coded:

        @pl.loop(0, chunks)
        def _(i):
            collect(i)

    for k in range(1, replicas):
        weight_copy(k, me).wait_send()
    for k in range(rounds):
        exchange(k, None).wait_send()
    for way in range(2):
        for hop in range(shards - 1):
            holds = jnp.logical_and(has_target(way), has_source(way, hop))
            if coded:
                less = outward(way)

                @pl.when(jnp.logical_and(holds, less))
                def _(way=way, hop=hop):
                    gather(way, hop, 0, chunks - spares // 2).wait_send()

                holds = jnp.logical_and(holds, jnp.logical_not(less))

            @pl.when(holds)
            def _(way=way, hop=hop):
                gather(way, hop, 0, chunks).wait_send()

    if coded:

        @pl.when(at_end(z))
        def _():
            relay(0, 2 * spares).wait_send()
            share(0, 0, spares).wait_send()
            share(1, 0, spares // 2).wait_send()

        if leads:
            lead_copy().wait_send()
        pltpu.make_async_remote_copy(
            src_ref=beside, dst_ref=beside, send_sem=bsend, recv_sem=brecv.at[0],
            device_id={"replica": peer(1)}, device_id_type=MESH,
        ).wait_send()


def per_device(params, first_moment, second_moment, grads, push_weight):
    replicas, shards = lax.axis_size("replica"), lax.axis_size("shard")
    _, rows, cols = params.shape
    units = cols // 128
    chunks = max(n for n in range(1, CHUNKS + 1) if units % n == 0)
    chunk = cols // chunks
    sub = max(128 * n for n in range(1, SUB + 1) if chunk % (128 * n) == 0)
    load_group = LOAD_GROUP if chunks % LOAD_GROUP == 0 else 1
    plan, mixes = plan_of(replicas), mixes_of(replicas)
    rounds = len(plan)
    alternate = replicas == 8 and plan[-1][1] == 1 and not plan[-1][2] and shards > 2
    spares = max(chunks - SWIFT - FULL_TAIL, 0) // 8 * 2 if alternate else 0
    f32, bf16, dma = jnp.float32, jnp.bfloat16, pltpu.SemaphoreType.DMA
    anywhere = pl.BlockSpec(memory_space=pl.ANY)
    body = functools.partial(kernel, plan, mixes, replicas, shards, chunks, chunk, sub, load_group, spares)
    hops = max(shards - 1, 1)
    large = (params, first_moment, second_moment, grads)
    large = tuple(pltpu.with_memory_space_constraint(x, pltpu.HBM) for x in large)
    apart = (shards - 1) * rows
    folding = (
        pltpu.VMEM((shards * rows, cols), bf16),
        pltpu.VMEM((apart, cols), bf16),
        pltpu.VMEM((apart, 8 * chunk), f32),
        pltpu.VMEM((apart, cols), bf16),
        pltpu.VMEM((2, apart, cols), bf16),
        pltpu.VMEM((apart, SWIFT * chunk), bf16),
        dma,
        dma((chunks,)),
        dma((2,)),
        dma((2, chunks)),
        dma,
        dma((SWIFT * (shards - 1),)),
        pltpu.VMEM((2, rows, chunk), bf16),
        dma,
        dma,
    )
    return pl.pallas_call(
        body,
        out_shape=jax.ShapeDtypeStruct((1, rows * shards, cols), bf16),
        in_specs=[anywhere] * 4 + [pl.BlockSpec(memory_space=pltpu.SMEM)],
        out_specs=pl.BlockSpec(memory_space=pltpu.VMEM),
        scratch_shapes=[
            pltpu.VMEM((rows, cols), f32),
            pltpu.VMEM((rows, cols), f32),
            pltpu.VMEM((rows, cols), f32),
            pltpu.VMEM((STEPS, rows, cols), bf16),
            pltpu.VMEM((replicas, 8, 128), f32),
            pltpu.VMEM((STEPS + 4, rows, sub), f32),
            pltpu.VMEM((rows, cols), f32),
            pltpu.VMEM((max(rounds - 1, 1), rows, cols), f32),
            pltpu.VMEM((max(plan[0][0], 1), rows, EARLY * chunk), f32),
            pltpu.VMEM((rounds, rows, cols), bf16),
            pltpu.VMEM((rounds, rows, cols), bf16),
            pltpu.VMEM((rows, cols), bf16),
            dma((4, chunks // load_group)),
            dma((replicas - 1,)),
            dma((replicas - 1,)),
            dma((rounds,)),
            dma((rounds, chunks)),
            dma((2, hops)),
            dma((2, hops, chunks)),
            *(folding if spares else ()),
        ],
        compiler_params=pltpu.CompilerParams(
            collective_id=0, has_side_effects=True, vmem_limit_bytes=48 * 1024 * 1024
        ),
    )(*large, push_weight)


def solution(mesh):
    return jax.shard_map(
        per_device,
        mesh=mesh,
        in_specs=(
            P("replica", "shard", None),
            P("replica", "shard", None),
            P("replica", "shard", None),
            P(None, "replica", "shard", None),
            P("replica"),
        ),
        out_specs=P("replica", None, None),
        check_vma=False,
    )
```

```python
import functools

import jax
import jax.numpy as jnp
from jax import lax
from jax.experimental import pallas as pl
from jax.experimental.pallas import tpu as pltpu
from jax.sharding import PartitionSpec as P

STEPS = 4


beta_one = 0.9
beta_two = 0.95
learn_rate = 0.1
decay_rate = 0.1
epsilon = 1e-08
adam_offset = 101

CODE_SCALE = 8.0
GAP_SCALE = 16.0
LAG = 3
HOP_LAG = 3
NEXT_HOP_LAG = 3
CHUNKS = 28
OPEN_LAG = 20
FOLD_LAG = 3
SWIFT = 1
SWIFT_AT = 17
SWIFT_LAG = 3
FULL_TAIL = 3
EAGER = 17
EARLY = 2
LOAD_GROUP = 4
SUB = 4
MESH = pl.DeviceIdType.MESH


def plan_of(replicas):
    levels = replicas.bit_length() - 1
    distances = [2 ** (step % levels) for step in range(STEPS)]
    every = {2**level for level in range(levels)}
    plan = []
    for step, distance in enumerate(distances):
        later = set(distances[step + 1 :])
        if every <= later:
            continue
        above = {d for d in every if d > distance}
        plan.append((step, distance, above <= later))
    return plan


def mixes_of(replicas):
    levels = replicas.bit_length() - 1
    mixes = [{0: 1.0}]
    for step in range(STEPS):
        distance, mixed = 2 ** (step % levels), {}
        for k, share in mixes[-1].items():
            for back in (k, (k + distance) % replicas):
                mixed[back] = mixed.get(back, 0.0) + 0.5 * share
        mixes.append(mixed)
    return mixes


def hop_lag(hop):
    return HOP_LAG + (hop - 1) * NEXT_HOP_LAG if hop else 0


def encode(value, scale=CODE_SCALE):
    power = value * scale
    power = power * power
    power = power * power
    power = power * power
    power = power * power
    return jnp.where(value < 0.0, -power, power).astype(jnp.bfloat16)


def decode(code, scale=CODE_SCALE):
    code = code.astype(jnp.float32)
    size = jnp.exp(jnp.log(jnp.abs(code)) * (1.0 / 16.0)) * (1.0 / scale)
    return jnp.where(code < 0.0, -size, size)


def kernel(
    plan, mixes, replicas, shards, chunks, chunk, sub, load_group, spares,
    params_ref, first_ref, second_ref, grads_ref, weight_ref, out_ref,
    params, first, second, grads, weights, scales, acc, terms, early, sent, arrived, final,
    load_sem, wsend, wrecv, xsend, xrecv, zsend, zrecv,
    codes=None, extra=None, hold=None, gap=None, gaps=None,
    beside=None,
    rsend=None, rrecv=None, gsend=None, grecv=None, bsend=None, brecv=None,
    lead=None, lsend=None, lrecv=None,
):
    me, z = lax.axis_index("replica"), lax.axis_index("shard")
    rows = params.shape[0]
    rounds = len(plan)
    ends = [step for step, _, _ in plan]
    keep = 1.0 - learn_rate * decay_rate
    coded = spares > 0
    swift = SWIFT if coded else 0
    leads = coded and ends[0] == 1 and plan[0][2]
    side, column, line = lax.rem(me, 2), lax.rem(me // 2, 2), me // 4
    foreign = shards - 1

    def columns(i):
        return pl.ds(pl.multiple_of(i * chunk, chunk), chunk)

    def spread(count):
        return pl.ds(0, count * chunk)

    def at_end(z):
        return jnp.logical_or(z == 0, z == shards - 1)

    def spared(i):
        return jnp.logical_and(i >= swift, i < swift + 4 * spares)

    def same_column(i):
        return lax.rem(i - swift, 2) == column

    def same_line(i):
        return lax.rem((i - swift) // 2, 2) == line

    def folded_here(i):
        return lax.rem((i - swift) // 4, 2) == side

    def everything(*tests):
        return functools.reduce(jnp.logical_and, tests)

    def lacking(i):
        return everything(spared(i), folded_here(i), same_column(i), same_line(i))

    def slab(index):
        return pl.ds(pl.multiple_of(index * rows, rows), rows)

    def peer(offset):
        return lax.rem(me + offset + replicas, replicas)

    barrier = pltpu.get_barrier_semaphore()
    for k in range(1, replicas):
        pl.semaphore_signal(barrier, inc=1, device_id={"replica": peer(k)}, device_id_type=MESH)

    @pl.when(z > 0)
    def _():
        pl.semaphore_signal(barrier, inc=1, device_id={"shard": z - 1}, device_id_type=MESH)

    @pl.when(z < shards - 1)
    def _():
        pl.semaphore_signal(barrier, inc=1, device_id={"shard": z + 1}, device_id_type=MESH)

    def loads(g):
        cols = pl.ds(pl.multiple_of(g * (load_group * chunk), chunk), load_group * chunk)
        return (
            pltpu.make_async_copy(params_ref.at[0, :, cols], params.at[:, cols], load_sem.at[0, g]),
            pltpu.make_async_copy(first_ref.at[0, :, cols], first.at[:, cols], load_sem.at[1, g]),
            pltpu.make_async_copy(second_ref.at[0, :, cols], second.at[:, cols], load_sem.at[2, g]),
            pltpu.make_async_copy(grads_ref.at[:, 0, :, cols], grads.at[:, :, cols], load_sem.at[3, g]),
        )

    @pl.loop(0, chunks // load_group)
    def _(g):
        for copy in loads(g):
            copy.start()

    weights[me] = jnp.full(weights.shape[1:], weight_ref[0], jnp.float32)
    ends_of_line = jnp.where(z > 0, 1, 0) + jnp.where(z < shards - 1, 1, 0)
    pl.semaphore_wait(barrier, replicas - 1 + ends_of_line)

    def weight_copy(k, owner):
        return pltpu.make_async_remote_copy(
            src_ref=weights.at[owner], dst_ref=weights.at[owner],
            send_sem=wsend.at[k - 1], recv_sem=wrecv.at[k - 1],
            device_id={"replica": peer(k)}, device_id_type=MESH,
        )

    for k in range(1, replicas):
        weight_copy(k, me).start()

    def wide(tile):
        tile = jnp.concatenate([tile] * (rows // tile.shape[0]), axis=0) if rows > tile.shape[0] else tile[:rows]
        return jnp.concatenate([tile] * (sub // tile.shape[1]), axis=1)

    heard = set()

    def mixed(level):
        total = None
        for k, share in sorted(mixes[level].items()):
            if k and k not in heard:
                weight_copy(k, peer(-k)).wait_recv()
                heard.add(k)
            part = share * weights[peer(-k)]
            total = part if total is None else total + part
        return total

    def scale_of(step):
        end = min(e for e in ends if e >= step)
        scales[1 + step] = wide(mixed(step) * (learn_rate * keep ** (end - step)))

    def partner(k):
        _, distance, swap = plan[k]
        return me + distance - 2 * distance * lax.rem(me // distance, 2) if swap else peer(distance)

    def lead_copy():
        return pltpu.make_async_remote_copy(
            src_ref=lead.at[0], dst_ref=lead.at[1], send_sem=lsend, recv_sem=lrecv,
            device_id={"replica": partner(0)}, device_id_type=MESH,
        )

    def start_early():
        for cols in tiles(0):
            sent[0, :, cols] = encode(acc[:, cols])
            lead[0, :, cols] = encode(early[0, :, cols])
        exchange(0, 0).start()
        lead_copy().start()

    def finish_early():
        lead_copy().wait_recv()
        for cols in tiles(0):
            acc[:, cols] = acc[:, cols] - decode(lead[1, :, cols]) * scales[3 + STEPS]

    def exchange(k, i):
        to = partner(k)
        cols = slice(None) if i is None else columns(i)
        return pltpu.make_async_remote_copy(
            src_ref=sent.at[k, :, cols], dst_ref=arrived.at[k, :, cols],
            send_sem=xsend.at[k], recv_sem=xrecv.at[k, 0 if i is None else i],
            device_id={"replica": to}, device_id_type=MESH,
        )

    def ring(index, cols):
        return codes.at[slab(index), cols] if coded else out_ref.at[0, slab(index), cols]

    def gather(way, hop, i, count=None, early=False):
        sign = 1 - 2 * way
        cols, index = columns(i) if count is None else spread(count), z - sign * hop
        target = ring(index, cols)
        return pltpu.make_async_remote_copy(
            src_ref=target if hop else sent.at[rounds - 1, :, cols] if early else final.at[:, cols], dst_ref=target,
            send_sem=zsend.at[way, hop], recv_sem=zrecv.at[way, hop, i],
            device_id={"shard": z + sign}, device_id_type=MESH,
        )

    def gathered(way, hop, i):
        sign = 1 - 2 * way
        target = ring(z - sign * hop, columns(i))
        return pltpu.make_async_remote_copy(
            src_ref=target, dst_ref=target,
            send_sem=zsend.at[way, hop - 1], recv_sem=zrecv.at[way, hop - 1, i],
            device_id={"shard": z - sign}, device_id_type=MESH,
        )

    def outward(way):
        return z == shards - 2 if way == 0 else z == 1

    def eager(way, i):
        return jnp.logical_or(i < EAGER, jnp.logical_not(outward(way))) if coded else i >= 0

    def sends(way, hop, i):
        holds = jnp.logical_and(has_target(way), has_source(way, hop))
        if coded:
            holds = jnp.logical_and(holds, jnp.logical_not(jnp.logical_and(outward(way), lacking(i))))
        return holds

    def has_source(way, hop):
        return z >= hop if way == 0 else z + hop < shards

    def has_target(way):
        return z < shards - 1 if way == 0 else z > 0

    def adam(cols, known):
        m, v = first[:, cols], second[:, cols]
        total = scales[0] * params[:, cols]
        for step in range(STEPS):
            g = grads[step, :, cols].astype(jnp.float32)
            count = adam_offset + step
            m = beta_one * m + (1.0 - beta_one) * g
            v = beta_two * v + (1.0 - beta_two) * g * g
            fixed = jnp.sqrt(v * (1.0 / (1.0 - beta_two**count))) + epsilon
            update = m * (1.0 / (1.0 - beta_one**count)) / fixed
            if step > ends[0]:
                terms[step - ends[0] - 1, :, cols] = update
            elif step < known:
                total = total - update * scales[1 + step]
            else:
                early[step - known, :, cols] = update
        return total

    def tiles(i):
        for j in range(chunk // sub):
            yield pl.ds(pl.multiple_of(i * chunk + j * sub, sub), sub)

    def first_half(i):
        for cols in tiles(i):
            acc[:, cols] = adam(cols, 1)

    def second_half(i):
        for cols in tiles(i):
            total = acc[:, cols]
            for step in range(1, ends[0] + 1):
                total = total - early[step - 1, :, cols] * scales[1 + step]
            acc[:, cols] = total
            if not (leads and i == 0):
                sent[0, :, cols] = encode(total)
        if not (leads and i == 0):
            exchange(0, i).start()

    def start_round(i):
        for cols in tiles(i):
            total = adam(cols, STEPS)
            acc[:, cols] = total
            sent[0, :, cols] = encode(total)
        exchange(0, i).start()

    def next_round(k, i):
        exchange(k - 1, i).wait_recv()
        if k == 1 and leads:
            pl.when(i == 0)(finish_early)
        for cols in tiles(i):
            both = acc[:, cols] + decode(arrived[k - 1, :, cols])
            if k < rounds:
                both = both * (0.5 * keep ** (ends[k] - ends[k - 1])) - terms[k - 1, :, cols] * scales[1 + ends[k]]
                acc[:, cols] = both
                sent[k, :, cols] = encode(both)
            else:
                done = (both * scales[1 + STEPS]).astype(jnp.bfloat16)
                out_ref[0, slab(z), cols] = done
                final[:, cols] = encode(0.5 * both) if coded else done
        if k < rounds:
            exchange(k, i).start()
            if k == rounds - 1 and swift:
                for way in range(2):
                    pl.when(jnp.logical_and(has_target(way), i < swift))(lambda way=way: gather(way, 0, i, early=True).start())
        else:
            for way in range(2):
                pl.when(everything(sends(way, 0, i), eager(way, i), i >= swift))(lambda way=way: gather(way, 0, i).start())

    def pass_on(hop, i):
        for way in range(2):

            @pl.when(everything(has_target(way), has_source(way, hop), eager(way, i)))
            def _(way=way):
                gathered(way, hop, i).wait_recv()

            @pl.when(everything(sends(way, hop, i), eager(way, i)))
            def _(way=way):
                gather(way, hop, i).start()

    def send_out(i):
        for way in range(2):

            @pl.when(everything(has_target(way), outward(way), i >= EAGER))
            def _(way=way):
                pl.when(sends(way, 0, i))(lambda: gather(way, 0, i).start())
                for hop in range(1, shards - 1):

                    @pl.when(has_source(way, hop))
                    def _(hop=hop):
                        gathered(way, hop, i).wait_recv()
                        pl.when(sends(way, hop, i))(lambda: gather(way, hop, i).start())

    def collect(i):
        for way in range(2):

            @pl.when(jnp.logical_not(has_target(way)))
            def _(way=way):
                for hop in range(1, shards):
                    gathered(way, hop, i).wait_recv()

    def abroad(j):
        return slab(j + jnp.where(j >= z, 1, 0))

    def relay(i, count=None):
        cols = columns(i) if count is None else spread(count)
        start = jnp.where(z == 0, rows, 0)
        return pltpu.make_async_remote_copy(
            src_ref=codes.at[pl.ds(pl.multiple_of(start, rows), foreign * rows), cols], dst_ref=extra.at[:, cols],
            send_sem=rsend, recv_sem=rrecv.at[i],
            device_id={"replica": me + 1 - 2 * side}, device_id_type=MESH,
        )

    def share(hop, i, count=None):
        cols = columns(i) if count is None else spread(count)
        to = me + 2 - 4 * column if hop else me + 4 - 8 * line
        return pltpu.make_async_remote_copy(
            src_ref=gap.at[:, cols], dst_ref=gaps.at[hop, :, cols],
            send_sem=gsend.at[hop], recv_sem=grecv.at[hop, i],
            device_id={"replica": to}, device_id_type=MESH,
        )

    def lend(i, j):
        return pltpu.make_async_remote_copy(
            src_ref=codes.at[abroad(j), columns(i)], dst_ref=beside.at[pl.ds(j * rows, rows), columns(i)],
            send_sem=bsend, recv_sem=brecv.at[i * foreign + j],
            device_id={"replica": peer(1)}, device_id_type=MESH,
        )

    def lend_swift(i):
        @pl.when(at_end(z))
        def _():
            collect(i)

        for j in range(foreign):
            lend(i, j).start()

    def open_swift(i):
        for j in range(foreign):
            lend(i, j).wait_recv()
        for at, where, cols, _ in foreign_tiles(i):
            both = decode(codes[where, cols]) + decode(beside[at, cols])
            out_ref[0, where, cols] = (both * scales[1 + STEPS]).astype(jnp.bfloat16)

    def foreign_tiles(i):
        for j in range(foreign):
            for cols, held in zip(tiles(i), tiles(lax.rem(i, 8))):
                yield pl.ds(j * rows, rows), abroad(j), cols, held

    def put(where, cols, value):
        out_ref[0, where, cols] = (value * scales[2 + STEPS]).astype(jnp.bfloat16)

    def open_slabs(i):
        folds = jnp.logical_and(at_end(z), spared(i))

        @pl.when(jnp.logical_and(at_end(z), jnp.logical_not(lacking(i))))
        def _():
            collect(i)

        @pl.when(jnp.logical_and(folds, jnp.logical_not(folded_here(i))))
        def _():
            relay(i).start()

        @pl.when(jnp.logical_not(jnp.logical_and(folds, folded_here(i))))
        def _():
            for _, where, cols, _ in foreign_tiles(i):
                put(where, cols, decode(codes[where, cols]))

    def begin_fold(i):
        @pl.when(everything(at_end(z), spared(i), folded_here(i), jnp.logical_not(lacking(i))))
        def _():
            relay(i).wait_recv()
            for at, where, cols, held in foreign_tiles(i):
                value = decode(codes[where, cols])
                put(where, cols, value)
                apart = decode(extra[at, cols]) - value
                hold[at, held] = apart
                gap[at, cols] = encode(apart, GAP_SCALE)

            @pl.when(jnp.logical_not(same_line(i)))
            def _():
                share(0, i).start()

    def join_fold(i):
        @pl.when(everything(at_end(z), spared(i), folded_here(i), same_line(i), jnp.logical_not(same_column(i))))
        def _():
            share(0, i).wait_recv()
            for at, _, cols, held in foreign_tiles(i):
                gap[at, cols] = encode(hold[at, held] + decode(gaps[0, at, cols], GAP_SCALE), GAP_SCALE)
            share(1, i).start()

    def end_fold(i):
        @pl.when(jnp.logical_and(at_end(z), lacking(i)))
        def _():
            relay(i).wait_recv()
            share(0, i).wait_recv()
            share(1, i).wait_recv()
            for at, where, cols, _ in foreign_tiles(i):
                apart = decode(gaps[0, at, cols], GAP_SCALE) + decode(gaps[1, at, cols], GAP_SCALE)
                put(where, cols, decode(extra[at, cols]) + apart)

    def wait_loads(i):
        @pl.when(lax.rem(i, load_group) == 0)
        def _():
            for copy in loads(i // load_group):
                copy.wait()

    scales[0] = wide(mixed(0) * keep ** (ends[0] + 1))
    scale_of(0)
    for i in range(EARLY):
        if i % load_group == 0:
            for copy in loads(i // load_group):
                copy.wait()
        first_half(i)
        if leads and i == 0:
            start_early()
    for step in range(1, ends[0] + 1):
        scale_of(step)
    for i in range(EARLY):
        second_half(i)
    wait_loads(EARLY)
    start_round(EARLY)
    for step in range(ends[0] + 1, STEPS):
        scale_of(step)
    scales[1 + STEPS] = wide(0.5 / mixed(STEPS))
    scales[2 + STEPS] = wide(1.0 / mixed(STEPS))
    if leads:
        theirs = sum(share * weights[lax.rem(partner(0) - k + replicas, replicas)] for k, share in mixes[1].items())
        scales[3 + STEPS] = wide(theirs * learn_rate)

    def catch_up(slot, final_slot, delay, act):
        until = jnp.where(slot == final_slot, 4 * spares + swift, slot - delay)

        @pl.when(jnp.logical_and(slot > delay, slot <= final_slot))
        def _():
            @pl.loop(slot - 1 - delay, until)
            def _(i):
                act(i)

    hops = max(shards - 2, 0)
    last = rounds * LAG
    late = max(last + hop_lag(hops), OPEN_LAG)

    @pl.loop(EARLY + 1, chunks + (late + 1 if coded else last + hop_lag(hops)))
    def _(t):
        def at(delay, act, low=0, high=chunks):
            i = t - delay

            @pl.when(jnp.logical_and(i >= low, i < high))
            def _():
                act(i)

        @pl.when(t < chunks)
        def _():
            wait_loads(t)
            start_round(t)

        for k in range(1, rounds + 1):
            at(k * LAG, functools.partial(next_round, k))
        for hop in range(1, hops + 1):
            at(last + hop_lag(hop), functools.partial(pass_on, hop), swift)
            if swift:
                at(last - LAG + hop_lag(hop), functools.partial(pass_on, hop), 0, swift)
        if coded:
            at(last + hop_lag(hops), send_out)
            at(late + 1, begin_fold)
            catch_up(t - late, chunks - 1, FOLD_LAG, join_fold)
            catch_up(t - late, chunks, 2 * FOLD_LAG, end_fold)
            at(late, open_slabs, swift)
            at(SWIFT_AT, lend_swift, 0, swift)
            at(SWIFT_AT + SWIFT_LAG, open_swift, 0, swift)

    if not coded:

        @pl.loop(0, chunks)
        def _(i):
            collect(i)

    for k in range(1, replicas):
        weight_copy(k, me).wait_send()
    for k in range(rounds):
        exchange(k, None).wait_send()
    for way in range(2):
        for hop in range(shards - 1):
            holds = jnp.logical_and(has_target(way), has_source(way, hop))
            if coded:
                less = outward(way)

                @pl.when(jnp.logical_and(holds, less))
                def _(way=way, hop=hop):
                    gather(way, hop, 0, chunks - spares // 2).wait_send()

                holds = jnp.logical_and(holds, jnp.logical_not(less))

            @pl.when(holds)
            def _(way=way, hop=hop):
                gather(way, hop, 0, chunks).wait_send()

    if coded:

        @pl.when(at_end(z))
        def _():
            relay(0, 2 * spares).wait_send()
            share(0, 0, spares).wait_send()
            share(1, 0, spares // 2).wait_send()

        if leads:
            lead_copy().wait_send()
        pltpu.make_async_remote_copy(
            src_ref=beside, dst_ref=beside, send_sem=bsend, recv_sem=brecv.at[0],
            device_id={"replica": peer(1)}, device_id_type=MESH,
        ).wait_send()


def per_device(params, first_moment, second_moment, grads, push_weight):
    replicas, shards = lax.axis_size("replica"), lax.axis_size("shard")
    _, rows, cols = params.shape
    units = cols // 128
    chunks = max(n for n in range(1, CHUNKS + 1) if units % n == 0)
    chunk = cols // chunks
    sub = max(128 * n for n in range(1, SUB + 1) if chunk % (128 * n) == 0)
    load_group = LOAD_GROUP if chunks % LOAD_GROUP == 0 else 1
    plan, mixes = plan_of(replicas), mixes_of(replicas)
    rounds = len(plan)
    alternate = replicas == 8 and plan[-1][1] == 1 and not plan[-1][2] and shards > 2
    spares = max(chunks - SWIFT - FULL_TAIL, 0) // 8 * 2 if alternate else 0
    f32, bf16, dma = jnp.float32, jnp.bfloat16, pltpu.SemaphoreType.DMA
    anywhere = pl.BlockSpec(memory_space=pl.ANY)
    body = functools.partial(kernel, plan, mixes, replicas, shards, chunks, chunk, sub, load_group, spares)
    hops = max(shards - 1, 1)
    large = (params, first_moment, second_moment, grads)
    large = tuple(pltpu.with_memory_space_constraint(x, pltpu.HBM) for x in large)
    apart = (shards - 1) * rows
    folding = (
        pltpu.VMEM((shards * rows, cols), bf16),
        pltpu.VMEM((apart, cols), bf16),
        pltpu.VMEM((apart, 8 * chunk), f32),
        pltpu.VMEM((apart, cols), bf16),
        pltpu.VMEM((2, apart, cols), bf16),
        pltpu.VMEM((apart, SWIFT * chunk), bf16),
        dma,
        dma((chunks,)),
        dma((2,)),
        dma((2, chunks)),
        dma,
        dma((SWIFT * (shards - 1),)),
        pltpu.VMEM((2, rows, chunk), bf16),
        dma,
        dma,
    )
    return pl.pallas_call(
        body,
        out_shape=jax.ShapeDtypeStruct((1, rows * shards, cols), bf16),
        in_specs=[anywhere] * 4 + [pl.BlockSpec(memory_space=pltpu.SMEM)],
        out_specs=pl.BlockSpec(memory_space=pltpu.VMEM),
        scratch_shapes=[
            pltpu.VMEM((rows, cols), f32),
            pltpu.VMEM((rows, cols), f32),
            pltpu.VMEM((rows, cols), f32),
            pltpu.VMEM((STEPS, rows, cols), bf16),
            pltpu.VMEM((replicas, 8, 128), f32),
            pltpu.VMEM((STEPS + 4, rows, sub), f32),
            pltpu.VMEM((rows, cols), f32),
            pltpu.VMEM((max(rounds - 1, 1), rows, cols), f32),
            pltpu.VMEM((max(plan[0][0], 1), rows, EARLY * chunk), f32),
            pltpu.VMEM((rounds, rows, cols), bf16),
            pltpu.VMEM((rounds, rows, cols), bf16),
            pltpu.VMEM((rows, cols), bf16),
            dma((4, chunks // load_group)),
            dma((replicas - 1,)),
            dma((replicas - 1,)),
            dma((rounds,)),
            dma((rounds, chunks)),
            dma((2, hops)),
            dma((2, hops, chunks)),
            *(folding if spares else ()),
        ],
        compiler_params=pltpu.CompilerParams(
            collective_id=0, has_side_effects=True, vmem_limit_bytes=48 * 1024 * 1024
        ),
    )(*large, push_weight)


def solution(mesh):
    return jax.shard_map(
        per_device,
        mesh=mesh,
        in_specs=(
            P("replica", "shard", None),
            P("replica", "shard", None),
            P("replica", "shard", None),
            P(None, "replica", "shard", None),
            P("replica"),
        ),
        out_specs=P("replica", None, None),
        check_vma=False,
    )
```

```python
import functools

import jax
import jax.numpy as jnp
from jax import lax
from jax.experimental import pallas as pl
from jax.experimental.pallas import tpu as pltpu
from jax.sharding import PartitionSpec as P

STEPS = 4


beta_one = 0.9
beta_two = 0.95
learn_rate = 0.1
decay_rate = 0.1
epsilon = 1e-08
adam_offset = 101

CODE_SCALE = 8.0
GAP_SCALE = 16.0
LAG = 3
HOP_LAG = 3
NEXT_HOP_LAG = 3
CHUNKS = 28
OPEN_LAG = 20
FOLD_LAG = 4
SWIFT = 1
SWIFT_AT = 17
SWIFT_LAG = 3
FULL_TAIL = 3
EAGER = 14
EARLY = 2
LOAD_GROUP = 4
SUB = 2
MESH = pl.DeviceIdType.MESH


def plan_of(replicas):
    levels = replicas.bit_length() - 1
    distances = [2 ** (step % levels) for step in range(STEPS)]
    every = {2**level for level in range(levels)}
    plan = []
    for step, distance in enumerate(distances):
        later = set(distances[step + 1 :])
        if every <= later:
            continue
        above = {d for d in every if d > distance}
        plan.append((step, distance, above <= later))
    return plan


def mixes_of(replicas):
    levels = replicas.bit_length() - 1
    mixes = [{0: 1.0}]
    for step in range(STEPS):
        distance, mixed = 2 ** (step % levels), {}
        for k, share in mixes[-1].items():
            for back in (k, (k + distance) % replicas):
                mixed[back] = mixed.get(back, 0.0) + 0.5 * share
        mixes.append(mixed)
    return mixes


def hop_lag(hop):
    return HOP_LAG + (hop - 1) * NEXT_HOP_LAG if hop else 0


def encode(value, scale=CODE_SCALE):
    power = value * scale
    power = power * power
    power = power * power
    power = power * power
    power = power * power
    return jnp.where(value < 0.0, -power, power).astype(jnp.bfloat16)


def decode(code, scale=CODE_SCALE):
    code = code.astype(jnp.float32)
    size = jnp.exp(jnp.log(jnp.abs(code)) * (1.0 / 16.0)) * (1.0 / scale)
    return jnp.where(code < 0.0, -size, size)


def kernel(
    plan, mixes, replicas, shards, chunks, chunk, sub, load_group, spares,
    params_ref, first_ref, second_ref, grads_ref, weight_ref, out_ref,
    params, first, second, grads, weights, scales, acc, terms, early, sent, arrived, final,
    load_sem, wsend, wrecv, xsend, xrecv, zsend, zrecv,
    codes=None, extra=None, hold=None, gap=None, gaps=None,
    beside=None,
    rsend=None, rrecv=None, gsend=None, grecv=None, bsend=None, brecv=None,
    lead=None, lsend=None, lrecv=None,
):
    me, z = lax.axis_index("replica"), lax.axis_index("shard")
    rows = params.shape[0]
    rounds = len(plan)
    ends = [step for step, _, _ in plan]
    keep = 1.0 - learn_rate * decay_rate
    coded = spares > 0
    swift = SWIFT if coded else 0
    leads = coded and ends[0] == 1 and plan[0][2]
    side, column, line = lax.rem(me, 2), lax.rem(me // 2, 2), me // 4
    foreign = shards - 1

    def columns(i):
        return pl.ds(pl.multiple_of(i * chunk, chunk), chunk)

    def spread(count):
        return pl.ds(0, count * chunk)

    def at_end(z):
        return jnp.logical_or(z == 0, z == shards - 1)

    def spared(i):
        return jnp.logical_and(i >= swift, i < swift + 4 * spares)

    def same_column(i):
        return lax.rem(i - swift, 2) == column

    def same_line(i):
        return lax.rem((i - swift) // 2, 2) == line

    def folded_here(i):
        return lax.rem((i - swift) // 4, 2) == side

    def everything(*tests):
        return functools.reduce(jnp.logical_and, tests)

    def lacking(i):
        return everything(spared(i), folded_here(i), same_column(i), same_line(i))

    def slab(index):
        return pl.ds(pl.multiple_of(index * rows, rows), rows)

    def peer(offset):
        return lax.rem(me + offset + replicas, replicas)

    barrier = pltpu.get_barrier_semaphore()
    for k in range(1, replicas):
        pl.semaphore_signal(barrier, inc=1, device_id={"replica": peer(k)}, device_id_type=MESH)

    @pl.when(z > 0)
    def _():
        pl.semaphore_signal(barrier, inc=1, device_id={"shard": z - 1}, device_id_type=MESH)

    @pl.when(z < shards - 1)
    def _():
        pl.semaphore_signal(barrier, inc=1, device_id={"shard": z + 1}, device_id_type=MESH)

    def loads(g):
        cols = pl.ds(pl.multiple_of(g * (load_group * chunk), chunk), load_group * chunk)
        return (
            pltpu.make_async_copy(params_ref.at[0, :, cols], params.at[:, cols], load_sem.at[0, g]),
            pltpu.make_async_copy(first_ref.at[0, :, cols], first.at[:, cols], load_sem.at[1, g]),
            pltpu.make_async_copy(second_ref.at[0, :, cols], second.at[:, cols], load_sem.at[2, g]),
            pltpu.make_async_copy(grads_ref.at[:, 0, :, cols], grads.at[:, :, cols], load_sem.at[3, g]),
        )

    @pl.loop(0, chunks // load_group)
    def _(g):
        for copy in loads(g):
            copy.start()

    weights[me] = jnp.full(weights.shape[1:], weight_ref[0], jnp.float32)
    ends_of_line = jnp.where(z > 0, 1, 0) + jnp.where(z < shards - 1, 1, 0)
    pl.semaphore_wait(barrier, replicas - 1 + ends_of_line)

    def weight_copy(k, owner):
        return pltpu.make_async_remote_copy(
            src_ref=weights.at[owner], dst_ref=weights.at[owner],
            send_sem=wsend.at[k - 1], recv_sem=wrecv.at[k - 1],
            device_id={"replica": peer(k)}, device_id_type=MESH,
        )

    for k in range(1, replicas):
        weight_copy(k, me).start()

    def wide(tile):
        tile = jnp.concatenate([tile] * (rows // tile.shape[0]), axis=0) if rows > tile.shape[0] else tile[:rows]
        return jnp.concatenate([tile] * (sub // tile.shape[1]), axis=1)

    heard = set()

    def mixed(level):
        total = None
        for k, share in sorted(mixes[level].items()):
            if k and k not in heard:
                weight_copy(k, peer(-k)).wait_recv()
                heard.add(k)
            part = share * weights[peer(-k)]
            total = part if total is None else total + part
        return total

    def scale_of(step):
        end = min(e for e in ends if e >= step)
        scales[1 + step] = wide(mixed(step) * (learn_rate * keep ** (end - step)))

    def partner(k):
        _, distance, swap = plan[k]
        return me + distance - 2 * distance * lax.rem(me // distance, 2) if swap else peer(distance)

    def lead_copy():
        return pltpu.make_async_remote_copy(
            src_ref=lead.at[0], dst_ref=lead.at[1], send_sem=lsend, recv_sem=lrecv,
            device_id={"replica": partner(0)}, device_id_type=MESH,
        )

    def start_early():
        for cols in tiles(0):
            sent[0, :, cols] = encode(acc[:, cols])
            lead[0, :, cols] = encode(early[0, :, cols])
        exchange(0, 0).start()
        lead_copy().start()

    def finish_early():
        lead_copy().wait_recv()
        for cols in tiles(0):
            acc[:, cols] = acc[:, cols] - decode(lead[1, :, cols]) * scales[3 + STEPS]

    def exchange(k, i):
        to = partner(k)
        cols = slice(None) if i is None else columns(i)
        return pltpu.make_async_remote_copy(
            src_ref=sent.at[k, :, cols], dst_ref=arrived.at[k, :, cols],
            send_sem=xsend.at[k], recv_sem=xrecv.at[k, 0 if i is None else i],
            device_id={"replica": to}, device_id_type=MESH,
        )

    def ring(index, cols):
        return codes.at[slab(index), cols] if coded else out_ref.at[0, slab(index), cols]

    def gather(way, hop, i, count=None, early=False):
        sign = 1 - 2 * way
        cols, index = columns(i) if count is None else spread(count), z - sign * hop
        target = ring(index, cols)
        return pltpu.make_async_remote_copy(
            src_ref=target if hop else sent.at[rounds - 1, :, cols] if early else final.at[:, cols], dst_ref=target,
            send_sem=zsend.at[way, hop], recv_sem=zrecv.at[way, hop, i],
            device_id={"shard": z + sign}, device_id_type=MESH,
        )

    def gathered(way, hop, i):
        sign = 1 - 2 * way
        target = ring(z - sign * hop, columns(i))
        return pltpu.make_async_remote_copy(
            src_ref=target, dst_ref=target,
            send_sem=zsend.at[way, hop - 1], recv_sem=zrecv.at[way, hop - 1, i],
            device_id={"shard": z - sign}, device_id_type=MESH,
        )

    def outward(way):
        return z == shards - 2 if way == 0 else z == 1

    def eager(way, i):
        return jnp.logical_or(i < EAGER, jnp.logical_not(outward(way))) if coded else i >= 0

    def sends(way, hop, i):
        holds = jnp.logical_and(has_target(way), has_source(way, hop))
        if coded:
            holds = jnp.logical_and(holds, jnp.logical_not(jnp.logical_and(outward(way), lacking(i))))
        return holds

    def has_source(way, hop):
        return z >= hop if way == 0 else z + hop < shards

    def has_target(way):
        return z < shards - 1 if way == 0 else z > 0

    def adam(cols, known):
        m, v = first[:, cols], second[:, cols]
        total = scales[0] * params[:, cols]
        for step in range(STEPS):
            g = grads[step, :, cols].astype(jnp.float32)
            count = adam_offset + step
            m = beta_one * m + (1.0 - beta_one) * g
            v = beta_two * v + (1.0 - beta_two) * g * g
            fixed = jnp.sqrt(v * (1.0 / (1.0 - beta_two**count))) + epsilon
            update = m * (1.0 / (1.0 - beta_one**count)) / fixed
            if step > ends[0]:
                terms[step - ends[0] - 1, :, cols] = update
            elif step < known:
                total = total - update * scales[1 + step]
            else:
                early[step - known, :, cols] = update
        return total

    def tiles(i):
        for j in range(chunk // sub):
            yield pl.ds(pl.multiple_of(i * chunk + j * sub, sub), sub)

    def first_half(i):
        for cols in tiles(i):
            acc[:, cols] = adam(cols, 1)

    def second_half(i):
        for cols in tiles(i):
            total = acc[:, cols]
            for step in range(1, ends[0] + 1):
                total = total - early[step - 1, :, cols] * scales[1 + step]
            acc[:, cols] = total
            if not (leads and i == 0):
                sent[0, :, cols] = encode(total)
        if not (leads and i == 0):
            exchange(0, i).start()

    def start_round(i):
        for cols in tiles(i):
            total = adam(cols, STEPS)
            acc[:, cols] = total
            sent[0, :, cols] = encode(total)
        exchange(0, i).start()

    def next_round(k, i):
        exchange(k - 1, i).wait_recv()
        if k == 1 and leads:
            pl.when(i == 0)(finish_early)
        for cols in tiles(i):
            both = acc[:, cols] + decode(arrived[k - 1, :, cols])
            if k < rounds:
                both = both * (0.5 * keep ** (ends[k] - ends[k - 1])) - terms[k - 1, :, cols] * scales[1 + ends[k]]
                acc[:, cols] = both
                sent[k, :, cols] = encode(both)
            else:
                done = (both * scales[1 + STEPS]).astype(jnp.bfloat16)
                out_ref[0, slab(z), cols] = done
                final[:, cols] = encode(0.5 * both) if coded else done
        if k < rounds:
            exchange(k, i).start()
            if k == rounds - 1 and swift:
                for way in range(2):
                    pl.when(jnp.logical_and(has_target(way), i < swift))(lambda way=way: gather(way, 0, i, early=True).start())
        else:
            for way in range(2):
                pl.when(everything(sends(way, 0, i), eager(way, i), i >= swift))(lambda way=way: gather(way, 0, i).start())

    def pass_on(hop, i):
        for way in range(2):

            @pl.when(everything(has_target(way), has_source(way, hop), eager(way, i)))
            def _(way=way):
                gathered(way, hop, i).wait_recv()

            @pl.when(everything(sends(way, hop, i), eager(way, i)))
            def _(way=way):
                gather(way, hop, i).start()

    def send_out(i):
        for way in range(2):

            @pl.when(everything(has_target(way), outward(way), i >= EAGER))
            def _(way=way):
                pl.when(sends(way, 0, i))(lambda: gather(way, 0, i).start())
                for hop in range(1, shards - 1):

                    @pl.when(has_source(way, hop))
                    def _(hop=hop):
                        gathered(way, hop, i).wait_recv()
                        pl.when(sends(way, hop, i))(lambda: gather(way, hop, i).start())

    def collect(i):
        for way in range(2):

            @pl.when(jnp.logical_not(has_target(way)))
            def _(way=way):
                for hop in range(1, shards):
                    gathered(way, hop, i).wait_recv()

    def abroad(j):
        return slab(j + jnp.where(j >= z, 1, 0))

    def relay(i, count=None):
        cols = columns(i) if count is None else spread(count)
        start = jnp.where(z == 0, rows, 0)
        return pltpu.make_async_remote_copy(
            src_ref=codes.at[pl.ds(pl.multiple_of(start, rows), foreign * rows), cols], dst_ref=extra.at[:, cols],
            send_sem=rsend, recv_sem=rrecv.at[i],
            device_id={"replica": me + 1 - 2 * side}, device_id_type=MESH,
        )

    def share(hop, i, count=None):
        cols = columns(i) if count is None else spread(count)
        to = me + 2 - 4 * column if hop else me + 4 - 8 * line
        return pltpu.make_async_remote_copy(
            src_ref=gap.at[:, cols], dst_ref=gaps.at[hop, :, cols],
            send_sem=gsend.at[hop], recv_sem=grecv.at[hop, i],
            device_id={"replica": to}, device_id_type=MESH,
        )

    def lend(i, j):
        return pltpu.make_async_remote_copy(
            src_ref=codes.at[abroad(j), columns(i)], dst_ref=beside.at[pl.ds(j * rows, rows), columns(i)],
            send_sem=bsend, recv_sem=brecv.at[i * foreign + j],
            device_id={"replica": peer(1)}, device_id_type=MESH,
        )

    def lend_swift(i):
        @pl.when(at_end(z))
        def _():
            collect(i)

        for j in range(foreign):
            lend(i, j).start()

    def open_swift(i):
        for j in range(foreign):
            lend(i, j).wait_recv()
        for at, where, cols, _ in foreign_tiles(i):
            both = decode(codes[where, cols]) + decode(beside[at, cols])
            out_ref[0, where, cols] = (both * scales[1 + STEPS]).astype(jnp.bfloat16)

    def foreign_tiles(i):
        for j in range(foreign):
            for cols, held in zip(tiles(i), tiles(lax.rem(i, 8))):
                yield pl.ds(j * rows, rows), abroad(j), cols, held

    def put(where, cols, value):
        out_ref[0, where, cols] = (value * scales[2 + STEPS]).astype(jnp.bfloat16)

    def open_slabs(i):
        folds = jnp.logical_and(at_end(z), spared(i))

        @pl.when(jnp.logical_and(at_end(z), jnp.logical_not(lacking(i))))
        def _():
            collect(i)

        @pl.when(jnp.logical_and(folds, jnp.logical_not(folded_here(i))))
        def _():
            relay(i).start()

        @pl.when(jnp.logical_not(jnp.logical_and(folds, folded_here(i))))
        def _():
            for _, where, cols, _ in foreign_tiles(i):
                put(where, cols, decode(codes[where, cols]))

    def begin_fold(i):
        @pl.when(everything(at_end(z), spared(i), folded_here(i), jnp.logical_not(lacking(i))))
        def _():
            relay(i).wait_recv()
            for at, where, cols, held in foreign_tiles(i):
                value = decode(codes[where, cols])
                put(where, cols, value)
                apart = decode(extra[at, cols]) - value
                hold[at, held] = apart
                gap[at, cols] = encode(apart, GAP_SCALE)

            @pl.when(jnp.logical_not(same_line(i)))
            def _():
                share(0, i).start()

    def join_fold(i):
        @pl.when(everything(at_end(z), spared(i), folded_here(i), same_line(i), jnp.logical_not(same_column(i))))
        def _():
            share(0, i).wait_recv()
            for at, _, cols, held in foreign_tiles(i):
                gap[at, cols] = encode(hold[at, held] + decode(gaps[0, at, cols], GAP_SCALE), GAP_SCALE)
            share(1, i).start()

    def end_fold(i):
        @pl.when(jnp.logical_and(at_end(z), lacking(i)))
        def _():
            relay(i).wait_recv()
            share(0, i).wait_recv()
            share(1, i).wait_recv()
            for at, where, cols, _ in foreign_tiles(i):
                apart = decode(gaps[0, at, cols], GAP_SCALE) + decode(gaps[1, at, cols], GAP_SCALE)
                put(where, cols, decode(extra[at, cols]) + apart)

    def wait_loads(i):
        @pl.when(lax.rem(i, load_group) == 0)
        def _():
            for copy in loads(i // load_group):
                copy.wait()

    scales[0] = wide(mixed(0) * keep ** (ends[0] + 1))
    scale_of(0)
    for i in range(EARLY):
        if i % load_group == 0:
            for copy in loads(i // load_group):
                copy.wait()
        first_half(i)
        if leads and i == 0:
            start_early()
    for step in range(1, ends[0] + 1):
        scale_of(step)
    for i in range(EARLY):
        second_half(i)
    wait_loads(EARLY)
    start_round(EARLY)
    for step in range(ends[0] + 1, STEPS):
        scale_of(step)
    scales[1 + STEPS] = wide(0.5 / mixed(STEPS))
    scales[2 + STEPS] = wide(1.0 / mixed(STEPS))
    if leads:
        theirs = sum(share * weights[lax.rem(partner(0) - k + replicas, replicas)] for k, share in mixes[1].items())
        scales[3 + STEPS] = wide(theirs * learn_rate)

    def catch_up(slot, final_slot, delay, act):
        until = jnp.where(slot == final_slot, 4 * spares + swift, slot - delay)

        @pl.when(jnp.logical_and(slot > delay, slot <= final_slot))
        def _():
            @pl.loop(slot - 1 - delay, until)
            def _(i):
                act(i)

    hops = max(shards - 2, 0)
    last = rounds * LAG
    late = max(last + hop_lag(hops), OPEN_LAG)

    @pl.loop(EARLY + 1, chunks + (late + 1 if coded else last + hop_lag(hops)))
    def _(t):
        def at(delay, act, low=0, high=chunks):
            i = t - delay

            @pl.when(jnp.logical_and(i >= low, i < high))
            def _():
                act(i)

        @pl.when(t < chunks)
        def _():
            wait_loads(t)
            start_round(t)

        for k in range(1, rounds + 1):
            at(k * LAG, functools.partial(next_round, k))
        for hop in range(1, hops + 1):
            at(last + hop_lag(hop), functools.partial(pass_on, hop), swift)
            if swift:
                at(last - LAG + hop_lag(hop), functools.partial(pass_on, hop), 0, swift)
        if coded:
            at(last + hop_lag(hops), send_out)
            at(late + 1, begin_fold)
            catch_up(t - late, chunks - 1, FOLD_LAG, join_fold)
            catch_up(t - late, chunks, 2 * FOLD_LAG, end_fold)
            at(late, open_slabs, swift)
            at(SWIFT_AT, lend_swift, 0, swift)
            at(SWIFT_AT + SWIFT_LAG, open_swift, 0, swift)

    if not coded:

        @pl.loop(0, chunks)
        def _(i):
            collect(i)

    for k in range(1, replicas):
        weight_copy(k, me).wait_send()
    for k in range(rounds):
        exchange(k, None).wait_send()
    for way in range(2):
        for hop in range(shards - 1):
            holds = jnp.logical_and(has_target(way), has_source(way, hop))
            if coded:
                less = outward(way)

                @pl.when(jnp.logical_and(holds, less))
                def _(way=way, hop=hop):
                    gather(way, hop, 0, chunks - spares // 2).wait_send()

                holds = jnp.logical_and(holds, jnp.logical_not(less))

            @pl.when(holds)
            def _(way=way, hop=hop):
                gather(way, hop, 0, chunks).wait_send()

    if coded:

        @pl.when(at_end(z))
        def _():
            relay(0, 2 * spares).wait_send()
            share(0, 0, spares).wait_send()
            share(1, 0, spares // 2).wait_send()

        if leads:
            lead_copy().wait_send()
        pltpu.make_async_remote_copy(
            src_ref=beside, dst_ref=beside, send_sem=bsend, recv_sem=brecv.at[0],
            device_id={"replica": peer(1)}, device_id_type=MESH,
        ).wait_send()


def per_device(params, first_moment, second_moment, grads, push_weight):
    replicas, shards = lax.axis_size("replica"), lax.axis_size("shard")
    _, rows, cols = params.shape
    units = cols // 128
    chunks = max(n for n in range(1, CHUNKS + 1) if units % n == 0)
    chunk = cols // chunks
    sub = max(128 * n for n in range(1, SUB + 1) if chunk % (128 * n) == 0)
    load_group = LOAD_GROUP if chunks % LOAD_GROUP == 0 else 1
    plan, mixes = plan_of(replicas), mixes_of(replicas)
    rounds = len(plan)
    alternate = replicas == 8 and plan[-1][1] == 1 and not plan[-1][2] and shards > 2
    spares = max(chunks - SWIFT - FULL_TAIL, 0) // 8 * 2 if alternate else 0
    f32, bf16, dma = jnp.float32, jnp.bfloat16, pltpu.SemaphoreType.DMA
    anywhere = pl.BlockSpec(memory_space=pl.ANY)
    body = functools.partial(kernel, plan, mixes, replicas, shards, chunks, chunk, sub, load_group, spares)
    hops = max(shards - 1, 1)
    large = (params, first_moment, second_moment, grads)
    large = tuple(pltpu.with_memory_space_constraint(x, pltpu.HBM) for x in large)
    apart = (shards - 1) * rows
    folding = (
        pltpu.VMEM((shards * rows, cols), bf16),
        pltpu.VMEM((apart, cols), bf16),
        pltpu.VMEM((apart, 8 * chunk), f32),
        pltpu.VMEM((apart, cols), bf16),
        pltpu.VMEM((2, apart, cols), bf16),
        pltpu.VMEM((apart, SWIFT * chunk), bf16),
        dma,
        dma((chunks,)),
        dma((2,)),
        dma((2, chunks)),
        dma,
        dma((SWIFT * (shards - 1),)),
        pltpu.VMEM((2, rows, chunk), bf16),
        dma,
        dma,
    )
    return pl.pallas_call(
        body,
        out_shape=jax.ShapeDtypeStruct((1, rows * shards, cols), bf16),
        in_specs=[anywhere] * 4 + [pl.BlockSpec(memory_space=pltpu.SMEM)],
        out_specs=pl.BlockSpec(memory_space=pltpu.VMEM),
        scratch_shapes=[
            pltpu.VMEM((rows, cols), f32),
            pltpu.VMEM((rows, cols), f32),
            pltpu.VMEM((rows, cols), f32),
            pltpu.VMEM((STEPS, rows, cols), bf16),
            pltpu.VMEM((replicas, 8, 128), f32),
            pltpu.VMEM((STEPS + 4, rows, sub), f32),
            pltpu.VMEM((rows, cols), f32),
            pltpu.VMEM((max(rounds - 1, 1), rows, cols), f32),
            pltpu.VMEM((max(plan[0][0], 1), rows, EARLY * chunk), f32),
            pltpu.VMEM((rounds, rows, cols), bf16),
            pltpu.VMEM((rounds, rows, cols), bf16),
            pltpu.VMEM((rows, cols), bf16),
            dma((4, chunks // load_group)),
            dma((replicas - 1,)),
            dma((replicas - 1,)),
            dma((rounds,)),
            dma((rounds, chunks)),
            dma((2, hops)),
            dma((2, hops, chunks)),
            *(folding if spares else ()),
        ],
        compiler_params=pltpu.CompilerParams(
            collective_id=0, has_side_effects=True, vmem_limit_bytes=48 * 1024 * 1024
        ),
    )(*large, push_weight)


def solution(mesh):
    return jax.shard_map(
        per_device,
        mesh=mesh,
        in_specs=(
            P("replica", "shard", None),
            P("replica", "shard", None),
            P("replica", "shard", None),
            P(None, "replica", "shard", None),
            P("replica"),
        ),
        out_specs=P("replica", None, None),
        check_vma=False,
    )
```
